32 devices in a mesh: ctx: 8 (over z, core), head: 4 (over y, x).
Axes of the slice: x: 2, y: 2, z: 4, core: 2. Of those that a mesh axis runs over, the one named last changes fastest.
Arguments:
- stretch_keys: bfloat16 [4, 32768, 128], P('head', 'ctx'), may hold values from -6 to 6
- stretch_values: bfloat16 [4, 32768, 128], P('head', 'ctx'), may hold values from -6 to 6
- stretch_assign: int32 [4, 32768], P('head', 'ctx'), may hold values from 0 to 4095, as said below
- centroid_keys: float32 [4, 4096, 128], P('head'), may hold values from -3.5 to 3.5
- centroid_values: float32 [4, 4096, 128], P('head'), may hold values from -3 to 3
- cluster_counts: float32 [4, 4096], P('head'), may hold values from 64 to 1024
- cache_keys: bfloat16 [4, 65536, 128], P('head', 'ctx'), may hold values from -6 to 6
- cache_values: bfloat16 [4, 65536, 128], P('head', 'ctx'), may hold values from -6 to 6
- block_cluster: int32 [4, 4096], P('head', 'ctx'), may hold values from 0 to 4095
- selected: int32 [4, 4, 64], P(None, 'head'), may hold values from 0 to 4095
- queries: bfloat16 [4, 64, 4, 128], P(None, 'head'), may hold values from -90 to 90
Outputs:
- new_keys: float32 [4, 4096, 128], P('head', 'ctx')
- new_values: float32 [4, 4096, 128], P('head', 'ctx')
- new_counts: float32 [4, 4096], P('head', 'ctx')
- attended: bfloat16 [4, 4, 64, 128], P(None, 'head', 'ctx')
The draws below stay inside these ranges and needn't reach their ends.
Inputs may be any that keep to these rules, and one draw needn't show every extreme that they name: `stretch_assign`: within each aligned block of 4096 prefill positions of one head, the clusters of one group j // (4096 / 8) are named at most 640 times; in every block some group is named exactly 640 times.
All inputs are finite; a program needn't handle non-finite values.
Results may differ from the reference program's by a relative error of at most 0.0045.
Values may be sent and summed in bfloat16 or wider, within the bound.
No kernel may reach another device: no remote copies, remote signals or barrier semaphores. Data moves between devices by JAX's collectives and lax.ppermute only.
A program may use at most 128 MiB of HBM per device.

```python
import math
import jax
import jax.numpy as jnp
from jax import lax

HD = 128
CLUSTERS = 4096
TOK_DEV = 4096
BLK = 16
SEL = 64
STEPS = 4
QROWS = 64
HEADS = 4
STRETCH = 32768
CONTEXT = 65536
NBLK = 4096
N_CTX = 8


def paired_draw(key):
    first = jax.random.fold_in(key, 11)
    second = jax.random.fold_in(key, 12)
    centre = jnp.clip(0.3 * jax.random.normal(first, (HEADS, CLUSTERS, HD), jnp.float32), -1.8, 1.8)
    query = jnp.clip(3.5 * jax.random.normal(second, (STEPS, QROWS, HEADS, HD), jnp.float32), -21.0, 21.0)
    return (centre, query)


def draw_centroid_keys(key, part):
    centre, query = paired_draw(key)
    return centre


def draw_queries(key, part):
    centre, query = paired_draw(key)
    return query.astype(jnp.bfloat16)


def assign_block(key):
    base = TOK_DEV // N_CTX
    extra = TOK_DEV // (4 * N_CTX)
    owned = CLUSTERS // N_CTX
    key_heavy, key_light, key_order, key_inner = jax.random.split(key, 4)
    heavy = jax.random.randint(key_heavy, (), 0, N_CTX, dtype=jnp.int32)
    light = (heavy + jax.random.randint(key_light, (), 1, N_CTX, dtype=jnp.int32)) % N_CTX
    owners = jnp.arange(N_CTX, dtype=jnp.int32)
    amounts = base + extra * (owners == heavy).astype(jnp.int32) - extra * (owners == light).astype(jnp.int32)
    bounds = jnp.cumsum(amounts)
    positions = jnp.arange(TOK_DEV, dtype=jnp.int32)
    owner = jnp.sum((positions[:, None] >= bounds[None, :]).astype(jnp.int32), axis=1)
    owner = jax.random.permutation(key_order, owner)
    inner = jax.random.randint(key_inner, (TOK_DEV,), 0, owned, dtype=jnp.int32)
    return owner * owned + inner


def draw_stretch_assign(key, part):
    keys = jax.random.split(jax.random.fold_in(key, 21), HEADS * N_CTX)
    return jax.vmap(assign_block)(keys).reshape(HEADS, STRETCH)


def place_ends(result, rng, smallest, top_value):
    longest = result.shape.index(max(result.shape))
    spots = []
    for shift in (0, 1):
        where = [jax.random.randint(jax.random.fold_in(rng, axis), (), 0, length) for axis, length in enumerate(result.shape)]
        where[longest] = (where[longest] + shift) % result.shape[longest]
        spots.append(tuple(where))
    return result.at[spots[0]].set(smallest).at[spots[1]].set(top_value)


def shard_levels(stream_key, dims, cuts, smallest, high):
    def one(axis_at, shards_of):
        heights = jax.random.uniform(jax.random.fold_in(jax.random.fold_in(stream_key, 6), axis_at), (shards_of,), jnp.float32, smallest / len(cuts), high / len(cuts))
        return jnp.repeat(jnp.exp(heights), dims[axis_at] // shards_of).reshape((-1,) + (1,) * (len(dims) - axis_at - 1))

    gain = one(*cuts[0])
    for cut in cuts[1:]:
        gain = gain * one(*cut)
    return gain


def normal_values(stream_key, shape, deviation, most, pieces=(), held_as=jnp.bfloat16):
    values = deviation * jax.random.normal(stream_key, shape, jnp.float32)
    if pieces:
        values = values * shard_levels(stream_key, shape, pieces, -0.22, 0.18)
    return jnp.clip(values, -most, most).astype(held_as)


def setup_inputs(seed: int = 0) -> dict:
    key_list = jax.random.split(jax.random.key(seed), 12)
    stretch_keys = normal_values(key_list[0], (HEADS, STRETCH, HD), 1.0, 6.0, ((0, 4), (1, 8)))
    stretch_values = normal_values(key_list[1], (HEADS, STRETCH, HD), 1.0, 6.0, ((0, 4), (1, 8)))
    stretch_assign = draw_stretch_assign(jax.random.fold_in(key_list[11], 71), 0)
    centroid_keys = draw_centroid_keys(jax.random.fold_in(key_list[11], 71), 0)
    centroid_values = normal_values(key_list[4], (HEADS, CLUSTERS, HD), 0.5, 3.0, ((0, 4),), jnp.float32)
    cluster_counts = jnp.clip(jnp.exp(math.log(1024.0) - 2.7725887 * jax.random.uniform(key_list[5], (HEADS, CLUSTERS), jnp.float32) ** shard_levels(key_list[5], (HEADS, CLUSTERS), ((0, 4),), -0.2, 0.2)), 64.0, 1024.0)
    cache_keys = normal_values(key_list[6], (HEADS, CONTEXT, HD), 1.0, 6.0, ((0, 4), (1, 8)))
    cache_values = normal_values(key_list[7], (HEADS, CONTEXT, HD), 1.0, 6.0, ((0, 4), (1, 8)))
    block_cluster = place_ends(jax.random.randint(key_list[8], (HEADS, NBLK), 0, CLUSTERS), jax.random.fold_in(key_list[8], 1), 0, CLUSTERS - 1).astype(jnp.int32)
    selected = place_ends(jax.random.randint(key_list[9], (STEPS, HEADS, SEL), 0, CLUSTERS), jax.random.fold_in(key_list[9], 1), 0, CLUSTERS - 1).astype(jnp.int32)
    queries = draw_queries(jax.random.fold_in(key_list[11], 71), 0)
    return {"stretch_keys": stretch_keys, "stretch_values": stretch_values, "stretch_assign": stretch_assign, "centroid_keys": centroid_keys, "centroid_values": centroid_values, "cluster_counts": cluster_counts, "cache_keys": cache_keys, "cache_values": cache_values, "block_cluster": block_cluster, "selected": selected, "queries": queries}


def one_head(items):
    stretch_k, stretch_v, assign, cent_k, cent_v, counts, cache_k, cache_v, blocks, chosen, rows_q = items
    joined = jnp.concatenate([stretch_k, stretch_v], axis=1).astype(jnp.float32)
    sums = jax.ops.segment_sum(joined, assign, num_segments=CLUSTERS)
    added = jax.ops.segment_sum(jnp.ones(assign.shape, jnp.float32), assign, num_segments=CLUSTERS)
    total = counts + added
    new_k = (counts[:, None] * cent_k + sums[:, :HD]) / total[:, None]
    new_v = (counts[:, None] * cent_v + sums[:, HD:]) / total[:, None]
    block_hit = jnp.any(blocks[None, :, None] == chosen[:, None, :], axis=-1)
    cache_hit = jnp.repeat(block_hit, BLK, axis=1)
    stretch_hit = jnp.any(assign[None, :, None] == chosen[:, None, :], axis=-1)
    labels = jnp.arange(CLUSTERS, dtype=jnp.int32)
    centre_free = jnp.logical_not(jnp.any(labels[None, :, None] == chosen[:, None, :], axis=-1))
    scale = HD ** (-0.5)
    hp = lax.Precision.HIGHEST
    query = rows_q.astype(jnp.float32)
    s_cache = jnp.einsum('sqd,td->sqt', query, cache_k.astype(jnp.float32), precision=hp) * scale
    s_stretch = jnp.einsum('sqd,td->sqt', query, stretch_k.astype(jnp.float32), precision=hp) * scale
    s_centre = jnp.einsum('sqd,cd->sqc', query, new_k, precision=hp) * scale + jnp.log(total)[None, None, :]
    s_cache = jnp.where(cache_hit[:, None, :], s_cache, -1e+30)
    s_stretch = jnp.where(stretch_hit[:, None, :], s_stretch, -1e+30)
    s_centre = jnp.where(centre_free[:, None, :], s_centre, -1e+30)
    peak = jnp.maximum(jnp.maximum(jnp.max(s_cache, -1), jnp.max(s_stretch, -1)), jnp.max(s_centre, -1))
    p_cache = jnp.where(cache_hit[:, None, :], jnp.exp(s_cache - peak[..., None]), 0.0)
    p_stretch = jnp.where(stretch_hit[:, None, :], jnp.exp(s_stretch - peak[..., None]), 0.0)
    p_centre = jnp.where(centre_free[:, None, :], jnp.exp(s_centre - peak[..., None]), 0.0)
    whole = jnp.sum(p_cache, -1) + jnp.sum(p_stretch, -1) + jnp.sum(p_centre, -1)
    r_cache = lax.optimization_barrier(p_cache.astype(jnp.bfloat16)).astype(jnp.float32)
    r_stretch = lax.optimization_barrier(p_stretch.astype(jnp.bfloat16)).astype(jnp.float32)
    acc = jnp.einsum('sqt,td->sqd', r_cache, cache_v.astype(jnp.float32), precision=hp)
    acc = acc + jnp.einsum('sqt,td->sqd', r_stretch, stretch_v.astype(jnp.float32), precision=hp)
    acc = acc + jnp.einsum('sqc,cd->sqd', p_centre, new_v, precision=hp)
    out = (acc / whole[..., None]).astype(jnp.bfloat16)
    return (new_k, new_v, total, out)

def reference(stretch_keys, stretch_values, stretch_assign, centroid_keys, centroid_values, cluster_counts, cache_keys, cache_values, block_cluster, selected, queries):
    items = (stretch_keys, stretch_values, stretch_assign, centroid_keys, centroid_values, cluster_counts, cache_keys, cache_values, block_cluster, jnp.moveaxis(selected, 1, 0), jnp.moveaxis(queries, 2, 0))
    new_keys, new_values, new_counts, attended = lax.map(one_head, items)
    return (new_keys, new_values, new_counts, jnp.moveaxis(attended, 0, 1))
```

```python
import functools
import jax
import jax.numpy as jnp
from jax import lax
from jax.experimental import pallas as pl
from jax.experimental.pallas import tpu as pltpu
from jax.sharding import PartitionSpec as P

LANES = 128
TAIL = 16
NEG = -1e30


def member_of(ids, chosen):
    return jnp.any(ids[..., :, None] == chosen[..., None, :], axis=-1)


def full_spec(shape):
    return pl.BlockSpec(shape, lambda *_: (0,) * len(shape))


def count_body(mine_ref, other_ref, out_ref, *, rows):
    total = jnp.zeros((rows, LANES), jnp.float32)
    for ref in (mine_ref, other_ref):
        ids = ref[...]
        span = ids.shape[1]
        high = lax.broadcasted_iota(jnp.int32, (rows, span), 0) == ids // LANES
        low = lax.broadcasted_iota(jnp.int32, (LANES, span), 0) == ids % LANES
        total = total + lax.dot_general(
            high.astype(jnp.float32).astype(jnp.bfloat16),
            low.astype(jnp.float32).astype(jnp.bfloat16),
            (((1,), (1,)), ((), ())),
            preferred_element_type=jnp.float32,
        )
    out_ref[...] = total


def chip_counts(mine, other, clusters):
    rows = clusters // LANES
    return pl.pallas_call(
        functools.partial(count_body, rows=rows),
        out_shape=jax.ShapeDtypeStruct((rows, LANES), jnp.float32),
        name="chip_counts",
    )(mine, other)


def segment_body(
    slot_ref, ka, va, ia, kb, vb, ib, count_ref, out_ref, total, *, owned
):
    step = pl.program_id(0)
    base = slot_ref[0] * owned

    @pl.when(step == 0)
    def _():
        total[...] = jnp.zeros_like(total)

    for keys, values, ids in ((ka, va, ia), (kb, vb, ib)):
        span = keys.shape[0]
        near = (ids[0] - base).astype(jnp.int16)
        spots = lax.broadcasted_iota(jnp.int16, (owned, span), 0)
        hot = jnp.where(spots == near, jnp.bfloat16(1), jnp.bfloat16(0))
        rows = jnp.concatenate([keys[...], values[...]], axis=1)
        total[...] += jnp.dot(hot, rows, preferred_element_type=jnp.float32)

    @pl.when(step == pl.num_programs(0) - 1)
    def _():
        out_ref[:owned, :] = total[...].astype(out_ref.dtype)
        counts = count_ref[0]
        high = jnp.floor(counts * (1.0 / 256.0))
        low = counts - 256.0 * high
        lines = counts.shape[0]
        packed = jnp.concatenate([high, low], axis=1)
        packed = jnp.concatenate(
            [packed, jnp.zeros((TAIL - lines, 2 * LANES), jnp.float32)], axis=0
        )
        out_ref[owned:, :] = packed.astype(out_ref.dtype)


def segment_sums(slot, mine, other, counts, owned, dtype, name):
    ka, va, ia = mine
    kb, vb, ib = other
    positions, width = ka.shape
    span = min(512, positions)
    steps = positions // span
    lines = owned // LANES
    rows_spec = pl.BlockSpec((span, width), lambda i, s: (i, 0))
    ids_spec = pl.BlockSpec((1, 1, span), lambda i, s: (i, 0, 0))
    ia, ib = ia.reshape(steps, 1, span), ib.reshape(steps, 1, span)
    return pl.pallas_call(
        functools.partial(segment_body, owned=owned),
        grid_spec=pltpu.PrefetchScalarGridSpec(
            num_scalar_prefetch=1,
            grid=(steps,),
            in_specs=[
                rows_spec, rows_spec, ids_spec, rows_spec, rows_spec, ids_spec,
                pl.BlockSpec((1, lines, LANES), lambda i, s: (s[0], 0, 0)),
            ],
            out_specs=pl.BlockSpec((owned + TAIL, 2 * width), lambda i, s: (0, 0)),
            scratch_shapes=[pltpu.VMEM((owned, 2 * width), jnp.float32)],
        ),
        out_shape=jax.ShapeDtypeStruct((owned + TAIL, 2 * width), dtype),
        cost_estimate=pl.CostEstimate(
            flops=8 * positions * owned * width, bytes_accessed=8 * positions * width, transcendentals=0
        ),
        name=name,
    )(slot.reshape(1), ka, va, ia, kb, vb, ib, counts.reshape(-1, lines, LANES))


def relay_body(own_ref, came_ref, out_ref, *, owned, lines):
    out_ref[:owned, :] = (
        own_ref[:owned, :].astype(jnp.float32) + came_ref[:owned, :].astype(jnp.float32)
    ).astype(out_ref.dtype)
    tail_own = own_ref[owned:, :].astype(jnp.float32)
    tail_came = came_ref[owned:, :].astype(jnp.float32)
    out_ref[owned:, :] = jnp.concatenate(
        [tail_own[:lines], tail_came[:lines], tail_own[2 * lines :]], axis=0
    ).astype(out_ref.dtype)


def relay(own, came, owned):
    return pl.pallas_call(
        functools.partial(relay_body, owned=owned, lines=owned // LANES),
        out_shape=jax.ShapeDtypeStruct(own.shape, own.dtype),
        cost_estimate=pl.CostEstimate(flops=10**9, bytes_accessed=3 * own.size * 2, transcendentals=0),
        name="relay",
    )(own, came)


def dense_body(
    q_ref, kc, vc, bc, ks, vs, bs, peak_ref, whole_ref, acc_ref, *, scale, steps
):
    @pl.when(pl.program_id(0) == 0)
    def _():
        peak_ref[...] = jnp.full_like(peak_ref, NEG)
        whole_ref[...] = jnp.zeros_like(whole_ref)
        acc_ref[...] = jnp.zeros_like(acc_ref)

    rows = q_ref.shape[0] // steps
    query = q_ref[...]
    for keys, values, bias in ((kc, vc, bc), (ks, vs, bs)):
        scores = lax.dot_general(
            query, keys[...], (((1,), (1,)), ((), ())), preferred_element_type=jnp.float32
        )
        scores = scores * scale
        shift = bias[...]
        scores = jnp.concatenate(
            [scores[s * rows : (s + 1) * rows] + shift[s : s + 1] for s in range(steps)], axis=0
        )
        old = peak_ref[...]
        new = jnp.maximum(old, jnp.max(scores, axis=1, keepdims=True))
        weights = jnp.exp(scores - new)
        fade = jnp.exp(old - new)
        peak_ref[...] = new
        whole_ref[...] = whole_ref[...] * fade + jnp.sum(weights, axis=1, keepdims=True)
        acc_ref[...] = acc_ref[...] * fade + jnp.dot(
            weights.astype(jnp.bfloat16), values[...], preferred_element_type=jnp.float32
        )


def dense_part(query, cache_k, cache_v, cache_bias, near_k, near_v, near_bias):
    rows, width = query.shape
    steps = cache_bias.shape[0]
    far, near = cache_k.shape[0], near_k.shape[0]
    turns = 4
    column = jax.ShapeDtypeStruct((rows, 1), jnp.float32)

    def long(n):
        return pl.BlockSpec((n // turns, width), lambda i: (i, 0))

    def wide(n):
        return pl.BlockSpec((steps, n // turns), lambda i: (0, i))

    return pl.pallas_call(
        functools.partial(dense_body, scale=width ** (-0.5), steps=steps),
        grid=(turns,),
        in_specs=[
            full_spec((rows, width)), long(far), long(far), wide(far), long(near), long(near), wide(near),
        ],
        out_specs=[full_spec((rows, 1)), full_spec((rows, 1)), full_spec((rows, width))],
        out_shape=[column, column, jax.ShapeDtypeStruct((rows, width), jnp.float32)],
        cost_estimate=pl.CostEstimate(
            flops=4 * rows * (far + near) * width, bytes_accessed=4 * (far + near) * width,
            transcendentals=rows * (far + near),
        ),
        name="dense_part",
    )(query, cache_k, cache_v, cache_bias, near_k, near_v, near_bias)


def finish_body(
    me_ref, own_ref, *refs, owned, lines, steps, groups, scale, parcels
):
    came = refs[:parcels]
    (ck, cv, cc, bias_ref, q_ref, peak_ref, whole_ref, acc_ref,
     nk_ref, nv_ref, nc_ref, out_ref, res_ref) = refs[parcels:]
    width = ck.shape[1]
    hp = lax.Precision.HIGHEST
    sums = own_ref[:owned, :]
    tail = own_ref[owned:, :]
    for ref in came:
        sums = sums + ref[:owned, :].astype(jnp.float32)
        tail = tail + ref[owned:, :].astype(jnp.float32)
    pairs = 256.0 * tail[:, :LANES] + tail[:, LANES:]
    added = pairs[:lines] + pairs[lines : 2 * lines]
    old = cc[0]
    total = old + added
    nc_ref[0] = total
    eye = lax.broadcasted_iota(jnp.int32, (LANES, LANES), 0) == lax.broadcasted_iota(
        jnp.int32, (LANES, LANES), 1
    )

    def stand(row):
        return jnp.sum(jnp.where(eye, row, 0.0), axis=1, keepdims=True)

    old_col = jnp.concatenate([stand(old[i : i + 1]) for i in range(lines)], axis=0)
    new_col = jnp.concatenate([stand(total[i : i + 1]) for i in range(lines)], axis=0)
    new_k = (old_col * ck[...] + sums[:, :width]) / new_col
    new_v = (old_col * cv[...] + sums[:, width:]) / new_col
    nk_ref[...] = new_k
    nv_ref[...] = new_v
    logs = jnp.log(total)
    log_row = jnp.concatenate([logs[i : i + 1] for i in range(lines)], axis=1)
    scores = lax.dot_general(
        q_ref[...].astype(jnp.float32), new_k, (((1,), (1,)), ((), ())),
        precision=hp, preferred_element_type=jnp.float32,
    )
    scores = scores * scale + log_row
    rows_all = scores.shape[0]
    rows = rows_all // steps
    shift = bias_ref[...]
    scores = jnp.concatenate(
        [scores[s * rows : (s + 1) * rows] + shift[s : s + 1] for s in range(steps)], axis=0
    )
    before = peak_ref[...]
    peak = jnp.maximum(before, jnp.max(scores, axis=1, keepdims=True))
    weights = jnp.exp(scores - peak)
    fade = jnp.exp(before - peak)
    whole = whole_ref[...] * fade + jnp.sum(weights, axis=1, keepdims=True)
    acc = acc_ref[...] * fade + jnp.dot(
        weights, new_v, precision=hp, preferred_element_type=jnp.float32
    )
    res_ref[...] = acc / whole
    level = peak + jnp.log(whole)
    marks = [
        jnp.sum(jnp.where(eye, level[i * LANES : (i + 1) * LANES], 0.0), axis=0, keepdims=True)
        for i in range(rows_all // LANES)
    ]
    marks = jnp.concatenate(marks + [jnp.zeros((8 - len(marks), LANES), jnp.float32)], axis=0)
    share = rows // groups
    for g in range(groups):
        for s in range(steps):
            out_ref[g, s * share : (s + 1) * share, :] = res_ref[
                s * rows + g * share : s * rows + (g + 1) * share, :
            ]
        out_ref[g, steps * share :, :] = marks


def finish(me, own, came, cent_k, cent_v, counts, bias, query, dense, groups, owned):
    clusters, width = cent_k.shape
    rows = query.shape[0]
    steps = bias.shape[0]
    lines = owned // LANES
    height = steps * (rows // steps // groups) + 8
    payload = full_spec((owned + TAIL, 2 * width))
    mine = pl.BlockSpec((owned, width), lambda i, s: (s[0], 0))
    line = pl.BlockSpec((1, lines, LANES), lambda i, s: (s[0], 0, 0))
    first_line = pl.BlockSpec((1, lines, LANES), lambda i, s: (0, 0, 0))
    column = full_spec((rows, 1))
    f32 = jnp.float32
    return pl.pallas_call(
        functools.partial(
            finish_body, owned=owned, lines=lines, steps=steps, groups=groups,
            scale=width ** (-0.5), parcels=len(came),
        ),
        grid_spec=pltpu.PrefetchScalarGridSpec(
            num_scalar_prefetch=1,
            grid=(1,),
            in_specs=[payload] + [payload] * len(came) + [
                mine, mine, line, full_spec((steps, owned)), full_spec((rows, width)),
                column, column, full_spec((rows, width)),
            ],
            out_specs=[
                full_spec((owned, width)), full_spec((owned, width)), first_line,
                full_spec((groups, height, LANES)),
            ],
            scratch_shapes=[pltpu.VMEM((rows, width), f32)],
        ),
        out_shape=[
            jax.ShapeDtypeStruct((owned, width), f32),
            jax.ShapeDtypeStruct((owned, width), f32),
            jax.ShapeDtypeStruct((1, lines, LANES), f32),
            jax.ShapeDtypeStruct((groups, height, LANES), f32),
        ],
        name="finish",
    )(me.reshape(1), own, *came, cent_k, cent_v, counts.reshape(-1, lines, LANES), bias, query, *dense)


def blend_body(me_ref, in_ref, out_ref, *, steps, share, groups, rows):
    count = steps * share
    tiles = steps * rows // LANES
    spot = lax.broadcasted_iota(jnp.int32, (count, LANES), 0)
    lane = lax.broadcasted_iota(jnp.int32, (count, LANES), 1)
    wanted = (spot // share) * rows + me_ref[0] * share + spot % share
    picks = [wanted == lane + i * LANES for i in range(tiles)]
    levels = []
    for g in range(groups):
        level = jnp.zeros((count, LANES), jnp.float32)
        for i in range(tiles):
            level = level + jnp.where(picks[i], in_ref[g, count + i : count + i + 1, :], 0.0)
        levels.append(jnp.sum(level, axis=1, keepdims=True))
    top = functools.reduce(jnp.maximum, levels)
    parts = [jnp.exp(level - top) for level in levels]
    whole = functools.reduce(jnp.add, parts)
    acc = sum(part * in_ref[g, :count, :] for g, part in enumerate(parts))
    out_ref[...] = (acc / whole).astype(out_ref.dtype)


def blend(me, packets, steps, share, groups, rows):
    return pl.pallas_call(
        functools.partial(blend_body, steps=steps, share=share, groups=groups, rows=rows),
        in_specs=[
            pl.BlockSpec(memory_space=pltpu.SMEM), pl.BlockSpec(memory_space=pltpu.VMEM),
        ],
        out_shape=jax.ShapeDtypeStruct((steps * share, LANES), jnp.bfloat16),
        name="blend",
    )(me.reshape(1), packets)


def spread(pairs):
    return [(2 * a + core, 2 * b + core) for a, b in pairs for core in (0, 1)]


def shards(
    stretch_keys, stretch_values, stretch_assign, centroid_keys, centroid_values, cluster_counts,
    cache_keys, cache_values, block_cluster, selected, queries,
):
    clusters, width = centroid_keys.shape[1:]
    groups = lax.axis_size("ctx")
    me = lax.axis_index("ctx")
    owned = clusters // groups
    chips = groups // 2
    chip, core = me // 2, me % 2
    swap = [(i, i ^ 1) for i in range(groups)]

    mine = (stretch_keys[0], stretch_values[0], stretch_assign)
    other = tuple(lax.ppermute(a, "ctx", swap) for a in mine)
    counts = chip_counts(mine[2], other[2], clusters)

    def sums_for(target, dtype, name):
        return segment_sums(
            (2 * target + core).astype(jnp.int32), mine, other, counts, owned, dtype, name
        )

    def move(a, pairs):
        return lax.ppermute(a, "ctx", spread(pairs))

    bf16 = jnp.bfloat16
    if chips == 4:
        left = chip < 2
        end = jnp.logical_or(chip == 0, chip == 3)
        slot0 = sums_for(jnp.where(left, 3, 0), bf16, "slot0")
        first = move(slot0, [(0, 1), (3, 2)])
        slot1 = sums_for(jnp.where(left, 2, 1), bf16, "slot1")
        skip = move(slot1, [(0, 2), (3, 1)])
        across = move(slot1, [(1, 2), (2, 1)])
        slot2 = sums_for(jnp.where(left, jnp.where(end, 1, 0), jnp.where(end, 2, 3)), bf16, "slot2")
        beside = move(slot2, [(0, 1), (1, 0), (2, 3), (3, 2)])
        far = move(relay(slot0, first, owned), [(1, 3), (2, 0)])
        came = [skip, across, beside, far]
    else:
        came = []
        for d in range(1, chips):
            slot = sums_for((chip + d) % chips, bf16, f"slot{d}")
            came.append(move(slot, [(i, (i + d) % chips) for i in range(chips)]))
    own = sums_for(chip, jnp.float32, "slot_own")

    rows_q = lax.all_to_all(queries, "head", split_axis=2, concat_axis=1, tiled=True)
    steps, query_rows = rows_q.shape[:2]
    query = rows_q.reshape(steps * query_rows, width)
    chosen = selected[:, 0]
    block_len = cache_keys.shape[1] // block_cluster.shape[1]

    def bias_of(ids, want):
        hit = member_of(jnp.broadcast_to(ids, (steps,) + ids.shape), chosen)
        return jnp.where(hit == want, 0.0, NEG).astype(jnp.float32)

    cache_bias = jnp.repeat(bias_of(block_cluster[0], True), block_len, axis=1)
    near_bias = bias_of(stretch_assign[0], True)
    own_bias = bias_of(me * owned + jnp.arange(owned, dtype=jnp.int32), False)
    dense = dense_part(
        query, cache_keys[0], cache_values[0], cache_bias, mine[0], mine[1], near_bias
    )
    new_keys, new_values, new_counts, packets = finish(
        me.astype(jnp.int32), own, came, centroid_keys[0], centroid_values[0], cluster_counts,
        own_bias, query, dense, groups, owned,
    )
    packets = lax.all_to_all(packets, "ctx", split_axis=0, concat_axis=0, tiled=True)
    share = query_rows // groups
    result = blend(me.astype(jnp.int32), packets, steps, share, groups, query_rows)
    return (
        new_keys[None],
        new_values[None],
        new_counts.reshape(1, owned),
        result.reshape(steps, 1, share, width),
    )


def solution(mesh):
    in_specs = (
        P("head", "ctx", None),
        P("head", "ctx", None),
        P("head", "ctx"),
        P("head", None, None),
        P("head", None, None),
        P("head", None),
        P("head", "ctx", None),
        P("head", "ctx", None),
        P("head", "ctx"),
        P(None, "head", None),
        P(None, "head", None, None),
    )
    out_specs = (
        P("head", "ctx", None),
        P("head", "ctx", None),
        P("head", "ctx"),
        P(None, "head", "ctx", None),
    )
    return jax.shard_map(shards, mesh=mesh, in_specs=in_specs, out_specs=out_specs, check_vma=False)
```

```python
import functools
import math
import jax
import jax.numpy as jnp
from jax import lax
from jax.experimental import pallas as pl
from jax.experimental.pallas import tpu as pltpu
from jax.sharding import PartitionSpec as P


LANES = 128
TAIL = 16
NEG = -1e30
LOG2E = math.log2(math.e)


def vmem(count):
    return [pl.BlockSpec(memory_space=pltpu.VMEM)] * count


def smem(count):
    return [pl.BlockSpec(memory_space=pltpu.SMEM)] * count


def params(mib):
    return pltpu.CompilerParams(vmem_limit_bytes=mib * 2**20)


def cost(flops, moved=2**20):
    return pl.CostEstimate(flops=int(flops), bytes_accessed=int(moved), transcendentals=0)


def turn_body(me_ref, in_ref, *refs):
    outs, held = refs[:-1], refs[-1]
    heads = len(outs)
    held[...] = in_ref[...].astype(jnp.float32)
    for d, out_ref in enumerate(outs):
        head = lax.rem(me_ref[0] + d, heads)
        out_ref[...] = held[pl.ds(head, out_ref.shape[0], stride=heads), :].astype(out_ref.dtype)


def by_head(me, queries):
    steps, rows, heads, width = queries.shape
    return pl.pallas_call(
        turn_body,
        in_specs=smem(1) + vmem(1), out_specs=vmem(heads),
        out_shape=[jax.ShapeDtypeStruct((steps * rows, width), queries.dtype)] * heads,
        scratch_shapes=[pltpu.VMEM((steps * rows * heads, width), jnp.float32)],
        compiler_params=params(4), cost_estimate=cost(1e8),
        name="by_head",
    )(me.reshape(1), queries.reshape(steps * rows * heads, width))


def count_body(mine_ref, other_ref, out_ref, *, rows):
    total = jnp.zeros((rows, LANES), jnp.float32)
    for ref in (mine_ref, other_ref):
        ids = ref[...]
        span = ids.shape[1]
        upper = (ids // LANES).astype(jnp.int16)
        lower = (ids % LANES).astype(jnp.int16)
        high = lax.broadcasted_iota(jnp.int16, (rows, span), 0) == upper
        low = lax.broadcasted_iota(jnp.int16, (LANES, span), 0) == lower
        one, none = jnp.bfloat16(1), jnp.bfloat16(0)
        total = total + lax.dot_general(
            jnp.where(high, one, none), jnp.where(low, one, none),
            (((1,), (1,)), ((), ())), preferred_element_type=jnp.float32,
        )
    out_ref[...] = total


def chip_counts(mine, other, clusters):
    rows = clusters // LANES
    return pl.pallas_call(
        functools.partial(count_body, rows=rows),
        in_specs=vmem(2), out_specs=vmem(1)[0],
        out_shape=jax.ShapeDtypeStruct((rows, LANES), jnp.float32),
        compiler_params=params(8), cost_estimate=cost(1e9),
        name="chip_counts",
    )(mine, other)


def segment_body(slot_ref, *refs, owned, sources, started, counted):
    out_ref = refs[-1]
    base = slot_ref[0] * owned
    parts = [refs[3 * sources][...]] if started else []
    positions = refs[0].shape[0]
    span = min(2048, positions)
    for i in range(sources):
        keys, values, ids = refs[3 * i : 3 * i + 3]
        for at in range(0, positions, span):
            near = (ids[:, at : at + span] - base).astype(jnp.int16)
            spots = lax.broadcasted_iota(jnp.int16, (owned, span), 0)
            hot = jnp.where(spots == near, jnp.bfloat16(1), jnp.bfloat16(0))
            rows = jnp.concatenate([keys[at : at + span, :], values[at : at + span, :]], axis=1)
            parts.append(jnp.dot(hot, rows, preferred_element_type=jnp.float32))
    total = functools.reduce(jnp.add, parts)
    if not counted:
        out_ref[...] = total
        return
    out_ref[:owned, :] = total.astype(out_ref.dtype)
    counts = refs[3 * sources + started][slot_ref[0]]
    high = jnp.floor(counts * (1.0 / 256.0))
    low = counts - 256.0 * high
    lines = counts.shape[0]
    packed = jnp.concatenate([high, low], axis=1)
    packed = jnp.concatenate(
        [packed, jnp.zeros((TAIL - lines, 2 * LANES), jnp.float32)], axis=0
    )
    out_ref[owned:, :] = packed.astype(out_ref.dtype)


def segment_sums(slot, sources, start, counts, owned, dtype):
    positions, width = sources[0][0].shape
    lines = owned // LANES
    args = [slot.reshape(1)]
    for source in sources:
        args += source
    if start is not None:
        args.append(start)
    if counts is not None:
        args.append(counts.reshape(-1, lines, LANES))
    height = owned if counts is None else owned + TAIL
    return pl.pallas_call(
        functools.partial(
            segment_body, owned=owned, sources=len(sources), started=start is not None,
            counted=counts is not None,
        ),
        in_specs=smem(1) + vmem(len(args) - 1), out_specs=vmem(1)[0],
        out_shape=jax.ShapeDtypeStruct((height, 2 * width), dtype),
        compiler_params=params(12),
        cost_estimate=cost(4 * len(sources) * positions * owned * width),
    )(*args)


def relay_body(own_ref, came_ref, out_ref, *, owned, lines):
    out_ref[:owned, :] = (
        own_ref[:owned, :].astype(jnp.float32) + came_ref[:owned, :].astype(jnp.float32)
    ).astype(out_ref.dtype)
    tail_own = own_ref[owned:, :].astype(jnp.float32)
    tail_came = came_ref[owned:, :].astype(jnp.float32)
    out_ref[owned:, :] = jnp.concatenate(
        [tail_own[:lines], tail_came[:lines], tail_own[2 * lines :]], axis=0
    ).astype(out_ref.dtype)


def relay(own, came, owned):
    return pl.pallas_call(
        functools.partial(relay_body, owned=owned, lines=owned // LANES),
        in_specs=vmem(2), out_specs=vmem(1)[0],
        out_shape=jax.ShapeDtypeStruct(own.shape, own.dtype),
        compiler_params=params(8), cost_estimate=cost(1e9),
        name="relay",
    )(own, came)


def dense_body(
    me_ref, *refs, scale, steps, span, block_len, heads
):
    asked = refs[:heads]
    (kc, vc, blocks, ks, vs, ids, sel_ref,
    peak_ref, whole_ref, acc_ref, q_ref, own_ref, query, held, best, sums, cache_bias, near_bias) = refs[heads:]
    rows = q_ref.shape[0] // steps
    piece = rows // heads
    for d, ref in enumerate(asked):
        part = ref[...].astype(jnp.float32)
        source = lax.rem(me_ref[1] + heads - d, heads)
        for s in range(steps):
            at = pl.ds(pl.multiple_of(s * rows + source * piece, piece), piece)
            q_ref[at, :] = part[s * piece : (s + 1) * piece]
    query[...] = q_ref[...].astype(query.dtype)
    chosen = sel_ref.shape[1]
    eye = lax.broadcasted_iota(jnp.int32, (chosen, chosen), 0) == lax.broadcasted_iota(
        jnp.int32, (chosen, chosen), 1
    )
    wanted = [
        jnp.sum(jnp.where(eye, sel_ref[s : s + 1, :].astype(jnp.float32), 0.0), axis=1, keepdims=True)
        for s in range(steps)
    ]

    def hits(names, s):
        same = names.astype(jnp.float32) == wanted[s]
        return jnp.max(jnp.where(same, 1.0, 0.0), axis=0, keepdims=True)

    owned = own_ref.shape[1]
    mine = me_ref[0] * owned + lax.broadcasted_iota(jnp.int32, (1, owned), 1)
    for s in range(steps):
        own_ref[s : s + 1, :] = hits(mine, s) * NEG
        near_bias[s : s + 1, :] = (1.0 - hits(ids[...], s)) * NEG
        cache_bias[s : s + 1, :] = 1.0 - hits(blocks[...], s)

    per = span // block_len
    widen = jnp.where(
        lax.broadcasted_iota(jnp.int32, (per, span), 0)
        == lax.broadcasted_iota(jnp.int32, (per, span), 1) // block_len,
        1.0, 0.0,
    ).astype(jnp.bfloat16)
    best[...] = jnp.full_like(best, NEG)
    sums[...] = jnp.zeros_like(sums)
    acc_ref[...] = jnp.zeros_like(acc_ref)

    def score(keys, at, shift, base):
        found = lax.dot_general(
            query[...], keys[at, :], (((1,), (1,)), ((), ())), preferred_element_type=jnp.float32
        )
        found = found * scale
        found = jnp.concatenate(
            [found[s * rows : (s + 1) * rows] + shift[s : s + 1] for s in range(steps)], axis=0
        )
        held[:, pl.ds(pl.multiple_of(base + at.start, span), span)] = found
        top = best[...]
        for i in range(span // LANES):
            top = jnp.maximum(top, found[:, i * LANES : (i + 1) * LANES])
        best[...] = top

    def window(turn):
        return pl.ds(pl.multiple_of(turn * span, span), span)

    def score_cache(turn, carry):
        shift = cache_bias[:, pl.ds(pl.multiple_of(turn * per, per), per)].astype(jnp.bfloat16)
        shift = jnp.dot(shift, widen, preferred_element_type=jnp.float32) * NEG
        score(kc, window(turn), shift, 0)
        return carry

    def score_near(turn, carry):
        score(ks, window(turn), near_bias[:, window(turn)], kc.shape[0])
        return carry

    lax.fori_loop(0, kc.shape[0] // span, score_cache, 0)
    lax.fori_loop(0, ks.shape[0] // span, score_near, 0)
    peak = jnp.max(best[...], axis=1, keepdims=True)
    peak_ref[...] = peak
    best[...] = jnp.broadcast_to(peak, best.shape)

    def weigh(values, at, base):
        top = best[...]
        total = sums[...]
        pieces = []
        for i in range(span // LANES):
            lanes = pl.ds(pl.multiple_of(base + at.start + i * LANES, LANES), LANES)
            piece = jnp.exp2(held[:, lanes] - top)
            total = total + piece
            pieces.append(piece.astype(jnp.bfloat16))
        sums[...] = total
        acc_ref[...] += jnp.dot(
            jnp.concatenate(pieces, axis=1), values[at, :], preferred_element_type=jnp.float32
        )

    def weigh_cache(turn, carry):
        weigh(vc, window(turn), 0)
        return carry

    def weigh_near(turn, carry):
        weigh(vs, window(turn), kc.shape[0])
        return carry

    lax.fori_loop(0, kc.shape[0] // span, weigh_cache, 0)
    lax.fori_loop(0, ks.shape[0] // span, weigh_near, 0)
    whole_ref[...] = jnp.sum(sums[...], axis=1, keepdims=True)


def dense_part(me, head, asked, cache_k, cache_v, blocks, near_k, near_v, ids, chosen, owned):
    width = asked[0].shape[1]
    heads = len(asked)
    rows = heads * asked[0].shape[0]
    steps = chosen.shape[0]
    far, near = cache_k.shape[0], near_k.shape[0]
    f32 = jnp.float32
    square = jax.ShapeDtypeStruct((rows, width), f32)
    column = jax.ShapeDtypeStruct((rows, 1), f32)
    tile = pltpu.VMEM((rows, LANES), f32)
    return pl.pallas_call(
        functools.partial(
            dense_body, scale=width ** (-0.5) * LOG2E, steps=steps, span=min(2048, far, near),
            block_len=far // blocks.shape[1], heads=heads,
        ),
        in_specs=smem(1) + vmem(heads + 7), out_specs=vmem(5),
        out_shape=[column, column, square, square, jax.ShapeDtypeStruct((steps, owned), f32)],
        scratch_shapes=[
            pltpu.VMEM((rows, width), asked[0].dtype), pltpu.VMEM((rows, far + near), f32), tile, tile,
            pltpu.VMEM((steps, blocks.shape[1]), f32), pltpu.VMEM((steps, near), f32),
        ],
        compiler_params=params(24),
        cost_estimate=cost(4 * rows * (far + near) * width),
        name="dense_part",
    )(jnp.stack([me, head]), *asked, cache_k, cache_v, blocks, near_k, near_v, ids, chosen)


def finish_body(
    me_ref, own_ref, *refs, owned, lines, steps, groups, scale, parcels
):
    came = refs[:parcels]
    (ck, cv, cc, bias_ref, q_ref, peak_ref, whole_ref, acc_ref,
     nk_ref, nv_ref, nc_ref, out_ref, res_ref) = refs[parcels:]
    width = ck.shape[1]
    hp = lax.Precision.HIGHEST
    sums = own_ref[:owned, :]
    tail = own_ref[owned:, :]
    for ref in came:
        sums = sums + ref[:owned, :].astype(jnp.float32)
        tail = tail + ref[owned:, :].astype(jnp.float32)
    pairs = 256.0 * tail[:, :LANES] + tail[:, LANES:]
    added = pairs[:lines] + pairs[lines : 2 * lines]
    old = cc[0]
    total = old + added
    nc_ref[0] = total
    eye = lax.broadcasted_iota(jnp.int32, (LANES, LANES), 0) == lax.broadcasted_iota(
        jnp.int32, (LANES, LANES), 1
    )

    def stand(row):
        return jnp.sum(jnp.where(eye, row, 0.0), axis=1, keepdims=True)

    old_col = jnp.concatenate([stand(old[i : i + 1]) for i in range(lines)], axis=0)
    new_col = jnp.concatenate([stand(total[i : i + 1]) for i in range(lines)], axis=0)
    new_k = (old_col * ck[...] + sums[:, :width]) / new_col
    new_v = (old_col * cv[...] + sums[:, width:]) / new_col
    nk_ref[...] = new_k
    nv_ref[...] = new_v
    logs = jnp.log(total) * LOG2E
    log_row = jnp.concatenate([logs[i : i + 1] for i in range(lines)], axis=1)
    scores = lax.dot_general(
        q_ref[...], new_k, (((1,), (1,)), ((), ())),
        precision=hp, preferred_element_type=jnp.float32,
    )
    scores = scores * scale + log_row
    rows_all = scores.shape[0]
    rows = rows_all // steps
    shift = bias_ref[...]
    scores = jnp.concatenate(
        [scores[s * rows : (s + 1) * rows] + shift[s : s + 1] for s in range(steps)], axis=0
    )
    before = peak_ref[...]
    peak = jnp.maximum(before, jnp.max(scores, axis=1, keepdims=True))
    weights = jnp.exp2(scores - peak)
    fade = jnp.exp2(before - peak)
    whole = whole_ref[...] * fade + jnp.sum(weights, axis=1, keepdims=True)
    acc = acc_ref[...] * fade + jnp.dot(
        weights, new_v, precision=hp, preferred_element_type=jnp.float32
    )
    res_ref[...] = acc / whole
    level = peak + jnp.log(whole) * LOG2E
    marks = [
        jnp.sum(jnp.where(eye, level[i * LANES : (i + 1) * LANES], 0.0), axis=0, keepdims=True)
        for i in range(rows_all // LANES)
    ]
    marks = jnp.concatenate(marks + [jnp.zeros((8 - len(marks), LANES), jnp.float32)], axis=0)
    share = rows // groups
    for g in range(groups):
        for s in range(steps):
            out_ref[g, s * share : (s + 1) * share, :] = res_ref[
                s * rows + g * share : s * rows + (g + 1) * share, :
            ]
        out_ref[g, steps * share :, :] = marks


def finish(me, own, came, cent_k, cent_v, counts, bias, query, dense, groups, owned):
    width = cent_k.shape[1]
    rows = query.shape[0]
    steps = bias.shape[0]
    lines = owned // LANES
    height = steps * (rows // steps // groups) + 8
    f32 = jnp.float32
    args = [me.reshape(1), own, *came, cent_k, cent_v, counts, bias, query, *dense]
    return pl.pallas_call(
        functools.partial(
            finish_body, owned=owned, lines=lines, steps=steps, groups=groups,
            scale=width ** (-0.5) * LOG2E, parcels=len(came),
        ),
        in_specs=smem(1) + vmem(len(args) - 1), out_specs=vmem(4),
        scratch_shapes=[pltpu.VMEM((rows, width), f32)],
        out_shape=[
            jax.ShapeDtypeStruct((owned, width), f32),
            jax.ShapeDtypeStruct((owned, width), f32),
            jax.ShapeDtypeStruct((1, lines, LANES), f32),
            jax.ShapeDtypeStruct((groups, height, LANES), f32),
        ],
        compiler_params=params(16), cost_estimate=cost(4e9),
        name="finish",
    )(*args)


def blend_body(me_ref, in_ref, out_ref, *, steps, share, groups, rows):
    count = steps * share
    tiles = steps * rows // LANES
    spot = lax.broadcasted_iota(jnp.int32, (count, LANES), 0)
    lane = lax.broadcasted_iota(jnp.int32, (count, LANES), 1)
    wanted = (spot // share) * rows + me_ref[0] * share + spot % share
    picks = [wanted == lane + i * LANES for i in range(tiles)]
    levels = []
    for g in range(groups):
        level = jnp.zeros((count, LANES), jnp.float32)
        for i in range(tiles):
            level = level + jnp.where(picks[i], in_ref[g, count + i : count + i + 1, :], 0.0)
        levels.append(jnp.sum(level, axis=1, keepdims=True))
    top = functools.reduce(jnp.maximum, levels)
    parts = [jnp.exp2(level - top) for level in levels]
    whole = functools.reduce(jnp.add, parts)
    acc = sum(part * in_ref[g, :count, :] for g, part in enumerate(parts))
    out_ref[...] = (acc / whole).astype(out_ref.dtype)


def blend(me, packets, steps, share, groups, rows):
    return pl.pallas_call(
        functools.partial(blend_body, steps=steps, share=share, groups=groups, rows=rows),
        in_specs=smem(1) + vmem(1), out_specs=vmem(1)[0],
        out_shape=jax.ShapeDtypeStruct((steps * share, LANES), jnp.bfloat16),
        compiler_params=params(8),
        name="blend",
    )(me.reshape(1), packets)


def spread(pairs):
    return [(2 * a + core, 2 * b + core) for a, b in pairs for core in (0, 1)]


def shards(
    stretch_keys, stretch_values, stretch_assign, centroid_keys, centroid_values, cluster_counts,
    cache_keys, cache_values, block_cluster, selected, queries,
):
    clusters, width = centroid_keys.shape[1:]
    groups = lax.axis_size("ctx")
    me = lax.axis_index("ctx")
    owned = clusters // groups
    chips = groups // 2
    chip, core = me // 2, me % 2
    swap = [(i, i ^ 1) for i in range(groups)]

    mine = (stretch_keys[0], stretch_values[0], stretch_assign)
    other = tuple(lax.ppermute(a, "ctx", swap) for a in mine)
    counts = chip_counts(mine[2], other[2], clusters)

    def sums_for(target, dtype):
        spot = (2 * target + core).astype(jnp.int32)
        return segment_sums(spot, (mine, other), None, counts, owned, dtype)

    def move(a, pairs):
        return lax.ppermute(a, "ctx", spread(pairs))

    bf16 = jnp.bfloat16
    if chips == 4:
        left = chip < 2
        end = jnp.logical_or(chip == 0, chip == 3)
        spot = (2 * jnp.where(left, 3, 0) + core).astype(jnp.int32)
        slot0 = segment_sums(spot, (mine,), None, None, owned, jnp.float32)
        slot0 = segment_sums(spot, (other,), slot0, counts, owned, bf16)
        first = move(slot0, [(0, 1), (3, 2)])
        slot1 = sums_for(jnp.where(left, 2, 1), bf16)
        skip = move(slot1, [(0, 2), (3, 1)])
        across = move(slot1, [(1, 2), (2, 1)])
        slot2 = sums_for(jnp.where(left, jnp.where(end, 1, 0), jnp.where(end, 2, 3)), bf16)
        beside = move(slot2, [(0, 1), (1, 0), (2, 3), (3, 2)])
        passed = relay(slot0, first, owned)
        far = move(passed, [(1, 3), (2, 0)])
        came = [skip, across, beside, far]
    else:
        came = []
        for d in range(1, chips):
            slot = sums_for((chip + d) % chips, bf16)
            came.append(move(slot, [(i, (i + d) % chips) for i in range(chips)]))
    own = sums_for(chip, jnp.float32)

    heads = lax.axis_size("head")
    head = lax.axis_index("head")
    asked = list(by_head(head.astype(jnp.int32), queries))
    for d in range(1, heads):
        asked[d] = lax.ppermute(asked[d], "head", [(i, (i + d) % heads) for i in range(heads)])
    steps = queries.shape[0]
    query_rows = heads * queries.shape[1]
    *dense, query, own_bias = dense_part(
        me.astype(jnp.int32), head.astype(jnp.int32), asked, cache_keys[0], cache_values[0],
        block_cluster, *mine, selected[:, 0], owned,
    )
    new_keys, new_values, new_counts, packets = finish(
        me.astype(jnp.int32), own, came,
        lax.dynamic_slice_in_dim(centroid_keys[0], me * owned, owned, 0),
        lax.dynamic_slice_in_dim(centroid_values[0], me * owned, owned, 0),
        lax.dynamic_slice_in_dim(cluster_counts[0], me * owned, owned, 0).reshape(1, -1, LANES),
        own_bias, query, dense, groups, owned,
    )
    packets = lax.all_to_all(packets, "ctx", split_axis=0, concat_axis=0, tiled=True)
    share = query_rows // groups
    result = blend(me.astype(jnp.int32), packets, steps, share, groups, query_rows)
    return (
        new_keys[None],
        new_values[None],
        new_counts.reshape(1, owned),
        result.reshape(steps, 1, share, width),
    )


def solution(mesh):
    in_specs = (
        P("head", "ctx", None),
        P("head", "ctx", None),
        P("head", "ctx"),
        P("head", None, None),
        P("head", None, None),
        P("head", None),
        P("head", "ctx", None),
        P("head", "ctx", None),
        P("head", "ctx"),
        P(None, "head", None),
        P(None, "head", None, None),
    )
    out_specs = (
        P("head", "ctx", None),
        P("head", "ctx", None),
        P("head", "ctx"),
        P(None, "head", "ctx", None),
    )
    return jax.shard_map(shards, mesh=mesh, in_specs=in_specs, out_specs=out_specs, check_vma=False)
```

```python
import functools
import math
import jax
import jax.numpy as jnp
from jax import lax
from jax.experimental import pallas as pl
from jax.experimental.pallas import tpu as pltpu
from jax.sharding import PartitionSpec as P


LANES = 128
TAIL = 16
NEG = -1e30
LOG2E = math.log2(math.e)


def vmem(count):
    return [pl.BlockSpec(memory_space=pltpu.VMEM)] * count


def hbm(count):
    return [pl.BlockSpec(memory_space=pltpu.HBM)] * count


def smem(count):
    return [pl.BlockSpec(memory_space=pltpu.SMEM)] * count


def params(mib):
    return pltpu.CompilerParams(vmem_limit_bytes=mib * 2**20)


def cost(flops, moved=2**20):
    return pl.CostEstimate(flops=int(flops), bytes_accessed=int(moved), transcendentals=0)


def turn_body(head_ref, in_ref, *refs):
    outs, held = refs[:-1], refs[-1]
    heads = len(outs)
    held[...] = in_ref[...].astype(jnp.float32)
    for d, out_ref in enumerate(outs):
        head = lax.rem(head_ref[0] + d, heads)
        out_ref[...] = held[pl.ds(head, out_ref.shape[0], stride=heads), :].astype(out_ref.dtype)


def by_head(spot, queries):
    steps, rows, heads, width = queries.shape
    return pl.pallas_call(
        turn_body,
        in_specs=smem(1) + vmem(1), out_specs=vmem(heads),
        out_shape=[jax.ShapeDtypeStruct((steps * rows, width), queries.dtype)] * heads,
        scratch_shapes=[pltpu.VMEM((steps * rows * heads, width), jnp.float32)],
        compiler_params=params(4), cost_estimate=cost(1e8),
        name="by_head",
    )(spot[1], queries.reshape(steps * rows * heads, width))


def count_body(mine_ref, other_ref, out_ref, *, rows):
    total = jnp.zeros((rows, LANES), jnp.float32)
    for ref in (mine_ref, other_ref):
        ids = ref[...]
        span = ids.shape[1]
        upper = (ids // LANES).astype(jnp.int16)
        lower = (ids % LANES).astype(jnp.int16)
        high = lax.broadcasted_iota(jnp.int16, (rows, span), 0) == upper
        low = lax.broadcasted_iota(jnp.int16, (LANES, span), 0) == lower
        one, none = jnp.bfloat16(1), jnp.bfloat16(0)
        total = total + lax.dot_general(
            jnp.where(high, one, none), jnp.where(low, one, none),
            (((1,), (1,)), ((), ())), preferred_element_type=jnp.float32,
        )
    out_ref[...] = total


def chip_counts(mine, other, clusters):
    rows = clusters // LANES
    return pl.pallas_call(
        functools.partial(count_body, rows=rows),
        in_specs=vmem(2), out_specs=vmem(1)[0],
        out_shape=jax.ShapeDtypeStruct((rows, LANES), jnp.float32),
        compiler_params=params(8), cost_estimate=cost(1e9),
        name="chip_counts",
    )(mine, other)


def slot_of(spot_ref, turn, chips):
    chip, core = spot_ref[0] // 2, spot_ref[0] % 2
    target = chip ^ turn if chips == 4 else lax.rem(chip + turn, chips)
    return 2 * target + core


def segment_body(spot_ref, head_ref, *refs, owned, sources, started, counted, turn, chips):
    out_ref = refs[-1]
    slot = slot_of(spot_ref, turn, chips)
    base = slot * owned
    parts = [refs[3 * sources][...]] if started else []
    positions = refs[0].shape[0]
    span = min(2048, positions)
    for i in range(sources):
        keys, values, ids = refs[3 * i : 3 * i + 3]
        for at in range(0, positions, span):
            near = (ids[:, at : at + span] - base).astype(jnp.int16)
            spots = lax.broadcasted_iota(jnp.int16, (owned, span), 0)
            hot = jnp.where(spots == near, jnp.bfloat16(1), jnp.bfloat16(0))
            rows = jnp.concatenate([keys[at : at + span, :], values[at : at + span, :]], axis=1)
            parts.append(jnp.dot(hot, rows, preferred_element_type=jnp.float32))
    total = functools.reduce(jnp.add, parts)
    if not counted:
        out_ref[...] = total
        return
    out_ref[:owned, :] = total.astype(out_ref.dtype)
    counts = refs[3 * sources + started][slot]
    high = jnp.floor(counts * (1.0 / 256.0))
    low = counts - 256.0 * high
    lines = counts.shape[0]
    packed = jnp.concatenate([high, low], axis=1)
    packed = jnp.concatenate(
        [packed, jnp.zeros((TAIL - lines, 2 * LANES), jnp.float32)], axis=0
    )
    out_ref[owned:, :] = packed.astype(out_ref.dtype)


def segment_sums(spot, turn, chips, sources, start, counts, owned, dtype):
    positions, width = sources[0][0].shape
    lines = owned // LANES
    args = [*spot]
    for source in sources:
        args += source
    if start is not None:
        args.append(start)
    if counts is not None:
        args.append(counts.reshape(-1, lines, LANES))
    height = owned if counts is None else owned + TAIL
    return pl.pallas_call(
        functools.partial(
            segment_body, owned=owned, sources=len(sources), started=start is not None,
            counted=counts is not None, turn=turn, chips=chips,
        ),
        in_specs=smem(2) + vmem(len(args) - 2), out_specs=vmem(1)[0],
        out_shape=jax.ShapeDtypeStruct((height, 2 * width), dtype),
        compiler_params=params(12),
        cost_estimate=cost(4 * len(sources) * positions * owned * width),
    )(*args)


def home_body(spot_ref, ck_hbm, cv_hbm, *refs, owned, **sizes):
    sources = refs[:7]
    out_ref, ck, cv, sems = refs[7:]
    rows = pl.ds(pl.multiple_of(spot_ref[0] * owned, owned), owned)
    copies = [
        pltpu.make_async_copy(src.at[rows, :], dst, sems.at[i])
        for i, (src, dst) in enumerate(((ck_hbm, ck), (cv_hbm, cv)))
    ]
    for copy in copies:
        copy.start()
    segment_body(
        spot_ref, None, *sources, out_ref, owned=owned, sources=2, started=False, counted=True, **sizes
    )
    for copy in copies:
        copy.wait()


def home_sums(spot, chips, mine, other, counts, cent_k, cent_v, owned):
    positions, width = mine[0].shape
    f32 = jnp.float32
    lines = owned // LANES
    return pl.pallas_call(
        functools.partial(home_body, owned=owned, turn=0, chips=chips),
        in_specs=smem(1) + hbm(2) + vmem(7), out_specs=vmem(3),
        out_shape=[
            jax.ShapeDtypeStruct((owned + TAIL, 2 * width), f32),
            jax.ShapeDtypeStruct((owned, width), f32),
            jax.ShapeDtypeStruct((owned, width), f32),
        ],
        scratch_shapes=[pltpu.SemaphoreType.DMA((2,))],
        compiler_params=params(12), cost_estimate=cost(8 * positions * owned * width),
        name="home_sums",
    )(spot[0], cent_k, cent_v, *mine, *other, counts.reshape(-1, lines, LANES))


def relay_body(own_ref, came_ref, out_ref, *, owned, lines):
    out_ref[:owned, :] = (
        own_ref[:owned, :].astype(jnp.float32) + came_ref[:owned, :].astype(jnp.float32)
    ).astype(out_ref.dtype)
    tail_own = own_ref[owned:, :].astype(jnp.float32)
    tail_came = came_ref[owned:, :].astype(jnp.float32)
    out_ref[owned:, :] = jnp.concatenate(
        [tail_own[:lines], tail_came[:lines], tail_own[2 * lines :]], axis=0
    ).astype(out_ref.dtype)


def relay(own, came, owned):
    return pl.pallas_call(
        functools.partial(relay_body, owned=owned, lines=owned // LANES),
        in_specs=vmem(2), out_specs=vmem(1)[0],
        out_shape=jax.ShapeDtypeStruct(own.shape, own.dtype),
        compiler_params=params(8), cost_estimate=cost(1e9),
        name="relay",
    )(own, came)


def dense_body(
    spot_ref, head_ref, *refs, scale, steps, span, block_len, heads
):
    asked = refs[:heads]
    (kc, vc, blocks, ks, vs, ids, sel_ref,
    peak_ref, whole_ref, acc_ref, q_ref, own_ref, query, held, best, sums, cache_bias, cache_hit, near_bias, light,
    kept_k, kept_v, list_v, list_s, sem) = refs[heads:]
    rows = q_ref.shape[0] // steps
    piece = rows // heads
    for d, ref in enumerate(asked):
        part = ref[...].astype(jnp.float32)
        source = lax.rem(head_ref[0] + heads - d, heads)
        for s in range(steps):
            at = pl.ds(pl.multiple_of(s * rows + source * piece, piece), piece)
            q_ref[at, :] = part[s * piece : (s + 1) * piece]
    query[...] = q_ref[...].astype(query.dtype)
    chosen = sel_ref.shape[1]
    eye = lax.broadcasted_iota(jnp.int32, (chosen, chosen), 0) == lax.broadcasted_iota(
        jnp.int32, (chosen, chosen), 1
    )
    wanted = jnp.concatenate(
        [
            jnp.broadcast_to(
                jnp.sum(
                    jnp.where(eye, sel_ref[s : s + 1, :].astype(jnp.float32), 0.0),
                    axis=1, keepdims=True,
                ),
                (chosen, LANES),
            )
            for s in range(steps)
        ],
        axis=0,
    )
    wanted = wanted.astype(jnp.int32).astype(jnp.int16)
    tell = jnp.where(
        lax.broadcasted_iota(jnp.int32, (8, steps * chosen), 0)
        == lax.broadcasted_iota(jnp.int32, (8, steps * chosen), 1) // chosen,
        1.0, 0.0,
    ).astype(jnp.bfloat16)

    def missing(names):
        names = names.astype(jnp.int16)
        same = jnp.concatenate(
            [
                jnp.where(
                    wanted == names[:, i : i + LANES], jnp.bfloat16(1), jnp.bfloat16(0)
                )
                for i in range(0, names.shape[1], LANES)
            ],
            axis=1,
        )
        found = jnp.dot(tell, same, preferred_element_type=jnp.float32)
        return jnp.where(found[:steps] > 0.5, 0.0, 1.0)

    owned = own_ref.shape[1]
    mine = spot_ref[0] * owned + lax.broadcasted_iota(jnp.int32, (1, owned), 1)
    own_ref[...] = (1.0 - missing(mine)) * NEG
    found = 1.0 - missing(blocks[...])
    count = found.shape[1]
    live = jnp.max(found, axis=0, keepdims=True)
    down = lax.broadcasted_iota(jnp.int32, (count, count), 0)
    along = lax.broadcasted_iota(jnp.int32, (count, count), 1)
    one, none = jnp.bfloat16(1), jnp.bfloat16(0)
    ahead = jnp.dot(
        jnp.broadcast_to(live, (8, count)).astype(jnp.bfloat16),
        jnp.where((down < along).astype(jnp.int16) > 0, one, none),
        preferred_element_type=jnp.float32,
    )[:1]
    place = jnp.where(live > 0.5, ahead, -1.0).astype(jnp.int32)
    chart = jnp.where((place == down).astype(jnp.int16) > 0, one, none)
    names = lax.broadcasted_iota(jnp.int32, (1, count), 1)
    table = jnp.concatenate(
        [(names // 64).astype(jnp.float32), (names % 64).astype(jnp.float32), found]
        + [jnp.zeros((6 - steps, count), jnp.float32)],
        axis=0,
    )
    packed = lax.dot_general(
        table.astype(jnp.bfloat16), chart, (((1,), (1,)), ((), ())),
        preferred_element_type=jnp.float32,
    )
    cache_hit[...] = packed[2 : 2 + steps]
    total = jnp.broadcast_to(jnp.sum(live, axis=1, keepdims=True), (1, count))
    list_v[...] = jnp.concatenate([64.0 * packed[:1] + packed[1:2], total], axis=0).astype(jnp.int32)
    listing = pltpu.make_async_copy(list_v, list_s, sem)
    listing.start()
    for at in range(0, ids.shape[1], 1024):
        near_bias[:, at : at + 1024] = missing(ids[:, at : at + 1024]) * NEG

    per = span // block_len
    widen = jnp.where(
        lax.broadcasted_iota(jnp.int32, (per, span), 0)
        == lax.broadcasted_iota(jnp.int32, (per, span), 1) // block_len,
        1.0, 0.0,
    ).astype(jnp.bfloat16)
    best[...] = jnp.full_like(best, NEG)
    sums[...] = jnp.zeros_like(sums)
    acc_ref[...] = jnp.zeros_like(acc_ref)

    def score(keys, at, shift, base):
        size = at.size
        found = lax.dot_general(
            query[...], keys[at, :], (((1,), (1,)), ((), ())), preferred_element_type=jnp.float32
        )
        found = found * scale
        found = jnp.concatenate(
            [found[s * rows : (s + 1) * rows] + shift[s : s + 1] for s in range(steps)], axis=0
        )
        held[:, pl.ds(pl.multiple_of(base + at.start, size), size)] = found
        top = best[...]
        for i in range(size // LANES):
            top = jnp.maximum(top, found[:, i * LANES : (i + 1) * LANES])
        best[...] = top

    def window(turn, span=span):
        return pl.ds(pl.multiple_of(turn * span, span), span)

    def score_near(turn, carry):
        score(ks, window(turn), near_bias[:, window(turn)], 0)
        return carry

    near = ks.shape[0]
    lax.fori_loop(0, near // span, score_near, 0)
    listing.wait()
    lively = list_s[1, 0]
    part = min(512, span)
    turns = (lively * block_len + part - 1) // part

    @pl.when(turns > 0)
    def _():
        last = window(turns - 1, part)
        kept_k[last, :] = jnp.zeros((part, kept_k.shape[1]), kept_k.dtype)
        kept_v[last, :] = jnp.zeros((part, kept_v.shape[1]), kept_v.dtype)

    def keep(n, carry):
        source = window(list_s[0, n], block_len)
        target = window(n, block_len)
        kept_k[target, :] = kc[source, :]
        kept_v[target, :] = vc[source, :]
        return carry

    lax.fori_loop(0, lively, keep, 0)

    def shift_cache(turn, carry):
        hit = cache_hit[:, pl.ds(pl.multiple_of(turn * per, per), per)].astype(jnp.bfloat16)
        cache_bias[:, window(turn)] = (
            1.0 - jnp.dot(hit, widen, preferred_element_type=jnp.float32)
        ) * NEG
        return carry

    lax.fori_loop(0, (lively + per - 1) // per, shift_cache, 0)

    def score_cache(turn, carry):
        at = window(turn, part)
        score(kept_k, at, cache_bias[:, at], near)
        return carry

    lax.fori_loop(0, turns, score_cache, 0)
    peak = jnp.max(best[...], axis=1, keepdims=True)
    peak_ref[...] = peak
    best[...] = jnp.broadcast_to(peak, best.shape)

    def weigh(values, at, base):
        tall, size = 64, at.size
        for r in range(0, best.shape[0], tall):
            top = best[r : r + tall, :]
            total = sums[r : r + tall, :]
            for i in range(0, size, LANES):
                lanes = pl.ds(pl.multiple_of(base + at.start + i, LANES), LANES)
                piece = jnp.exp2(held[r : r + tall, lanes] - top)
                total = total + piece
                light[r : r + tall, i : i + LANES] = piece.astype(light.dtype)
            sums[r : r + tall, :] = total
        acc_ref[...] += jnp.dot(
            light[:, :size], values[at, :], preferred_element_type=jnp.float32
        )

    def weigh_near(turn, carry):
        weigh(vs, window(turn), 0)
        return carry

    def weigh_cache(turn, carry):
        weigh(kept_v, window(turn, part), near)
        return carry

    lax.fori_loop(0, near // span, weigh_near, 0)
    lax.fori_loop(0, turns, weigh_cache, 0)
    whole_ref[...] = jnp.sum(sums[...], axis=1, keepdims=True)


def dense_part(spot, asked, cache_k, cache_v, blocks, near_k, near_v, ids, chosen, owned):
    width = asked[0].shape[1]
    heads = len(asked)
    rows = heads * asked[0].shape[0]
    steps = chosen.shape[0]
    far, near = cache_k.shape[0], near_k.shape[0]
    f32 = jnp.float32
    square = jax.ShapeDtypeStruct((rows, width), f32)
    span = min(2048, far, near)
    column = jax.ShapeDtypeStruct((rows, 1), f32)
    tile = pltpu.VMEM((rows, LANES), f32)
    return pl.pallas_call(
        functools.partial(
            dense_body, scale=width ** (-0.5) * LOG2E, steps=steps, span=span,
            block_len=far // blocks.shape[1], heads=heads,
        ),
        in_specs=smem(2) + vmem(heads + 7), out_specs=vmem(5),
        out_shape=[column, column, square, square, jax.ShapeDtypeStruct((steps, owned), f32)],
        scratch_shapes=[
            pltpu.VMEM((rows, width), asked[0].dtype), pltpu.VMEM((rows, far + near), f32), tile, tile,
            pltpu.VMEM((steps, far), f32), pltpu.VMEM((steps, blocks.shape[1]), f32),
            pltpu.VMEM((steps, near), f32), pltpu.VMEM((rows, span), jnp.bfloat16),
            pltpu.VMEM((far, width), cache_k.dtype), pltpu.VMEM((far, width), cache_v.dtype),
            pltpu.VMEM((2, blocks.shape[1]), jnp.int32), pltpu.SMEM((2, blocks.shape[1]), jnp.int32),
            pltpu.SemaphoreType.DMA(()),
        ],
        compiler_params=params(24),
        cost_estimate=cost(4 * rows * (far + near) * width),
        name="dense_part",
    )(*spot, *asked, cache_k, cache_v, blocks, near_k, near_v, ids, chosen)


def pieces_of(value, count):
    out = []
    for _ in range(count):
        piece = value.astype(jnp.bfloat16)
        out.append(piece)
        value = value - piece.astype(jnp.float32)
    return out


def finish_body(
    spot_ref, own_ref, *refs, owned, lines, steps, groups, scale, parcels
):
    came = refs[:parcels]
    (ck, cv, cc, bias_ref, q_ref, peak_ref, whole_ref, acc_ref,
     nk_ref, nv_ref, nc_ref, out_ref, res_ref, held) = refs[parcels:]
    width = ck.shape[1]
    sums = own_ref[:owned, :]
    tail = own_ref[owned:, :]
    for ref in came:
        sums = sums + ref[:owned, :].astype(jnp.float32)
        tail = tail + ref[owned:, :].astype(jnp.float32)
    pairs = 256.0 * tail[:, :LANES] + tail[:, LANES:]
    added = pairs[:lines] + pairs[lines : 2 * lines]
    old_row = cc[:, pl.ds(pl.multiple_of(spot_ref[0] * owned, owned), owned)]
    total_row = old_row + jnp.concatenate([added[i : i + 1] for i in range(lines)], axis=1)
    nc_ref[...] = total_row
    eye = lax.broadcasted_iota(jnp.int32, (LANES, LANES), 0) == lax.broadcasted_iota(
        jnp.int32, (LANES, LANES), 1
    )

    def stand(row):
        return jnp.sum(jnp.where(eye, row, 0.0), axis=1, keepdims=True)

    def column(row):
        return jnp.concatenate(
            [stand(row[:, i : i + LANES]) for i in range(0, owned, LANES)], axis=0
        )

    old_col, new_col = column(old_row), column(total_row)
    new_k = (old_col * ck[...] + sums[:, :width]) / new_col
    new_v = (old_col * cv[...] + sums[:, width:]) / new_col
    nk_ref[...] = new_k
    nv_ref[...] = new_v
    log_row = jnp.log(total_row) * LOG2E
    query = q_ref[...].astype(jnp.bfloat16)
    scores = sum(
        lax.dot_general(
            query, piece, (((1,), (1,)), ((), ())), preferred_element_type=jnp.float32
        )
        for piece in reversed(pieces_of(new_k, 3))
    )
    scores = scores * scale + log_row
    rows_all = scores.shape[0]
    rows = rows_all // steps
    shift = bias_ref[...]
    scores = jnp.concatenate(
        [scores[s * rows : (s + 1) * rows] + shift[s : s + 1] for s in range(steps)], axis=0
    )
    before = peak_ref[...]
    peak = jnp.maximum(before, jnp.max(scores, axis=1, keepdims=True))
    weights = jnp.exp2(scores - peak)
    fade = jnp.exp2(before - peak)
    whole = whole_ref[...] * fade + jnp.sum(weights, axis=1, keepdims=True)
    (w_high, w_low), (v_high, v_low) = pieces_of(weights, 2), pieces_of(new_v, 2)
    acc = acc_ref[...] * fade
    for left, right in ((w_low, v_high), (w_high, v_low), (w_high, v_high)):
        acc = acc + jnp.dot(left, right, preferred_element_type=jnp.float32)
    res_ref[...] = acc / whole
    level = peak + jnp.log(whole) * LOG2E
    marks = [
        jnp.sum(jnp.where(eye, level[i * LANES : (i + 1) * LANES], 0.0), axis=0, keepdims=True)
        for i in range(rows_all // LANES)
    ]
    marks = [piece.astype(jnp.float32) for mark in marks for piece in pieces_of(mark, 3)]
    marks = jnp.concatenate(marks + [jnp.zeros((TAIL - len(marks), LANES), jnp.float32)], axis=0)
    share = rows // groups
    for g in range(groups):
        for s in range(steps):
            held[g, s * share : (s + 1) * share, :] = res_ref[
                s * rows + g * share : s * rows + (g + 1) * share, :
            ]
        held[g, steps * share :, :] = marks
    out_ref[...] = held[...].astype(out_ref.dtype)


def finish(spot, own, came, cent_k, cent_v, counts, bias, query, dense, groups, owned):
    width = cent_k.shape[1]
    rows = query.shape[0]
    steps = bias.shape[0]
    lines = owned // LANES
    height = steps * (rows // steps // groups) + TAIL
    f32 = jnp.float32
    args = [spot[0], own, *came, cent_k, cent_v, counts, bias, query, *dense]
    return pl.pallas_call(
        functools.partial(
            finish_body, owned=owned, lines=lines, steps=steps, groups=groups,
            scale=width ** (-0.5) * LOG2E, parcels=len(came),
        ),
        in_specs=smem(1) + vmem(len(args) - 1), out_specs=vmem(4),
        scratch_shapes=[
            pltpu.VMEM((rows, width), f32), pltpu.VMEM((groups, height, LANES), f32),
        ],
        out_shape=[
            jax.ShapeDtypeStruct((owned, width), f32),
            jax.ShapeDtypeStruct((owned, width), f32),
            jax.ShapeDtypeStruct((1, owned), f32),
            jax.ShapeDtypeStruct((groups, height, LANES), jnp.bfloat16),
        ],
        compiler_params=params(16), cost_estimate=cost(4e9),
        name="finish",
    )(*args)


def blend_body(spot_ref, in_ref, out_ref, *, steps, share, groups, rows):
    count = steps * share
    tiles = steps * rows // LANES
    spot = lax.broadcasted_iota(jnp.int32, (count, LANES), 0)
    lane = lax.broadcasted_iota(jnp.int32, (count, LANES), 1)
    wanted = (spot // share) * rows + spot_ref[0] * share + spot % share
    picks = [wanted == lane + i * LANES for i in range(tiles)]
    levels = []
    for g in range(groups):
        level = jnp.zeros((count, LANES), jnp.float32)
        marks = in_ref[g, count:, :].astype(jnp.float32)
        for i in range(tiles):
            mark = marks[3 * i : 3 * i + 1] + marks[3 * i + 1 : 3 * i + 2] + marks[3 * i + 2 : 3 * i + 3]
            level = level + jnp.where(picks[i], mark, 0.0)
        levels.append(jnp.sum(level, axis=1, keepdims=True))
    top = functools.reduce(jnp.maximum, levels)
    parts = [jnp.exp2(level - top) for level in levels]
    whole = functools.reduce(jnp.add, parts)
    acc = sum(part * in_ref[g, :count, :].astype(jnp.float32) for g, part in enumerate(parts))
    out_ref[...] = (acc / whole).astype(out_ref.dtype)


def blend(spot, packets, steps, share, groups, rows):
    return pl.pallas_call(
        functools.partial(blend_body, steps=steps, share=share, groups=groups, rows=rows),
        in_specs=smem(1) + vmem(1), out_specs=vmem(1)[0],
        out_shape=jax.ShapeDtypeStruct((steps * share, LANES), jnp.bfloat16),
        compiler_params=params(8),
        name="blend",
    )(spot[0], packets)


def spread(pairs):
    return [(2 * a + core, 2 * b + core) for a, b in pairs for core in (0, 1)]


def shards(
    stretch_keys, stretch_values, stretch_assign, centroid_keys, centroid_values, cluster_counts,
    cache_keys, cache_values, block_cluster, selected, queries,
):
    clusters, width = centroid_keys.shape[1:]
    groups = lax.axis_size("ctx")
    owned = clusters // groups
    chips = groups // 2
    swap = [(i, i ^ 1) for i in range(groups)]
    spot = tuple(lax.axis_index(name).astype(jnp.int32).reshape(1) for name in ("ctx", "head"))

    mine = (stretch_keys[0], stretch_values[0], stretch_assign)
    other = tuple(lax.ppermute(a, "ctx", swap) for a in mine)
    lead = 3 if chips == 4 else 1
    slot_a = segment_sums(spot, lead, chips, (mine,), None, None, owned, jnp.float32)
    counts = chip_counts(mine[2], other[2], clusters)
    slot_a = segment_sums(spot, lead, chips, (other,), slot_a, counts, owned, jnp.bfloat16)

    def sums_for(turn):
        return segment_sums(spot, turn, chips, (mine, other), None, counts, owned, jnp.bfloat16)

    def move(a, pairs):
        return lax.ppermute(a, "ctx", spread(pairs))

    if chips == 4:
        first = move(slot_a, [(0, 1), (3, 2)])
        across = move(slot_a, [(1, 2), (2, 1)])
        slot_b = sums_for(2)
        skip = move(slot_b, [(0, 2), (3, 1)])
        passed = relay(slot_b, first, owned)
        far = move(passed, [(1, 3), (2, 0)])
        slot_c = sums_for(1)
        beside = move(slot_c, [(0, 1), (1, 0), (2, 3), (3, 2)])
        came = [skip, across, beside, far]
    else:
        came = [move(slot_a, [(i, (i + 1) % chips) for i in range(chips)])]
        for d in range(2, chips):
            slot = sums_for(d)
            came.append(move(slot, [(i, (i + d) % chips) for i in range(chips)]))
    own, own_k, own_v = home_sums(
        spot, chips, mine, other, counts, centroid_keys[0], centroid_values[0], owned
    )
    heads = lax.axis_size("head")
    asked = list(by_head(spot, queries))
    for d in range(1, heads):
        asked[d] = lax.ppermute(asked[d], "head", [(i, (i + d) % heads) for i in range(heads)])
    steps = queries.shape[0]
    query_rows = heads * queries.shape[1]
    *dense, query, own_bias = dense_part(
        spot, asked, cache_keys[0], cache_values[0],
        block_cluster, *mine, selected[:, 0], owned,
    )
    new_keys, new_values, new_counts, packets = finish(
        spot, own, came, own_k, own_v, cluster_counts,
        own_bias, query, dense, groups, owned,
    )
    packets = lax.all_to_all(packets, "ctx", split_axis=0, concat_axis=0, tiled=True)
    share = query_rows // groups
    result = blend(spot, packets, steps, share, groups, query_rows)
    return (
        new_keys[None],
        new_values[None],
        new_counts,
        result.reshape(steps, 1, share, width),
    )


def solution(mesh):
    in_specs = (
        P("head", "ctx", None),
        P("head", "ctx", None),
        P("head", "ctx"),
        P("head", None, None),
        P("head", None, None),
        P("head", None),
        P("head", "ctx", None),
        P("head", "ctx", None),
        P("head", "ctx"),
        P(None, "head", None),
        P(None, "head", None, None),
    )
    out_specs = (
        P("head", "ctx", None),
        P("head", "ctx", None),
        P("head", "ctx"),
        P(None, "head", "ctx", None),
    )
    return jax.shard_map(shards, mesh=mesh, in_specs=in_specs, out_specs=out_specs, check_vma=False)
```

```python
import functools
import math
import jax
import jax.numpy as jnp
from jax import lax
from jax.experimental import pallas as pl
from jax.experimental.pallas import tpu as pltpu
from jax.sharding import PartitionSpec as P


LANES = 128
TAIL = 16
NEG = -1e30
LOG2E = math.log2(math.e)


def vmem(count):
    return [pl.BlockSpec(memory_space=pltpu.VMEM)] * count


def hbm(count):
    return [pl.BlockSpec(memory_space=pltpu.HBM)] * count


def smem(count):
    return [pl.BlockSpec(memory_space=pltpu.SMEM)] * count


def params(mib):
    return pltpu.CompilerParams(vmem_limit_bytes=mib * 2**20)


def cost(flops, moved=2**20):
    return pl.CostEstimate(flops=int(flops), bytes_accessed=int(moved), transcendentals=0)


def turn_body(head_ref, in_ref, *refs):
    outs, held = refs[:-1], refs[-1]
    heads = len(outs)
    held[...] = in_ref[...].astype(jnp.float32)
    for d, out_ref in enumerate(outs):
        head = lax.rem(head_ref[0] + d, heads)
        out_ref[...] = held[pl.ds(head, out_ref.shape[0], stride=heads), :].astype(out_ref.dtype)


def by_head(spot, queries):
    steps, rows, heads, width = queries.shape
    return pl.pallas_call(
        turn_body,
        in_specs=smem(1) + vmem(1), out_specs=vmem(heads),
        out_shape=[jax.ShapeDtypeStruct((steps * rows, width), queries.dtype)] * heads,
        scratch_shapes=[pltpu.VMEM((steps * rows * heads, width), jnp.float32)],
        compiler_params=params(4), cost_estimate=cost(1e8),
        name="by_head",
    )(spot[1], queries.reshape(steps * rows * heads, width))


def count_body(mine_ref, other_ref, out_ref, *, rows):
    total = jnp.zeros((rows, LANES), jnp.float32)
    for ref in (mine_ref, other_ref):
        ids = ref[...]
        span = ids.shape[1]
        upper = (ids // LANES).astype(jnp.int16)
        lower = (ids % LANES).astype(jnp.int16)
        high = lax.broadcasted_iota(jnp.int16, (rows, span), 0) == upper
        low = lax.broadcasted_iota(jnp.int16, (LANES, span), 0) == lower
        one, none = jnp.bfloat16(1), jnp.bfloat16(0)
        total = total + lax.dot_general(
            jnp.where(high, one, none), jnp.where(low, one, none),
            (((1,), (1,)), ((), ())), preferred_element_type=jnp.float32,
        )
    out_ref[...] = total


def chip_counts(mine, other, clusters):
    rows = clusters // LANES
    return pl.pallas_call(
        functools.partial(count_body, rows=rows),
        in_specs=vmem(2), out_specs=vmem(1)[0],
        out_shape=jax.ShapeDtypeStruct((rows, LANES), jnp.float32),
        compiler_params=params(8), cost_estimate=cost(1e9),
        name="chip_counts",
    )(mine, other)


def target_of(chip, turn, chips):
    return chip ^ turn if chips & (chips - 1) == 0 else (chip + turn) % chips


def slot_of(spot_ref, turn, chips):
    chip, core = spot_ref[0] // 2, spot_ref[0] % 2
    return 2 * target_of(chip, turn, chips) + core


def segment_body(spot_ref, head_ref, *refs, owned, sources, started, counted, turn, chips):
    out_ref = refs[-1]
    slot = slot_of(spot_ref, turn, chips)
    base = slot * owned
    parts = [refs[3 * sources][...]] if started else []
    positions = refs[0].shape[0]
    span = min(2048, positions)
    for i in range(sources):
        keys, values, ids = refs[3 * i : 3 * i + 3]
        for at in range(0, positions, span):
            near = (ids[:, at : at + span] - base).astype(jnp.int16)
            spots = lax.broadcasted_iota(jnp.int16, (owned, span), 0)
            hot = jnp.where(spots == near, jnp.bfloat16(1), jnp.bfloat16(0))
            rows = jnp.concatenate([keys[at : at + span, :], values[at : at + span, :]], axis=1)
            parts.append(jnp.dot(hot, rows, preferred_element_type=jnp.float32))
    total = functools.reduce(jnp.add, parts)
    if not counted:
        out_ref[...] = total
        return
    out_ref[:owned, :] = total.astype(out_ref.dtype)
    counts = refs[3 * sources + started][slot]
    high = jnp.floor(counts * (1.0 / 256.0))
    low = counts - 256.0 * high
    lines = counts.shape[0]
    packed = jnp.concatenate([high, low], axis=1)
    packed = jnp.concatenate(
        [packed, jnp.zeros((TAIL - lines, 2 * LANES), jnp.float32)], axis=0
    )
    out_ref[owned:, :] = packed.astype(out_ref.dtype)


def segment_sums(spot, turn, chips, sources, start, counts, owned, dtype, after=None):
    positions, width = sources[0][0].shape
    lines = owned // LANES
    args = [*spot]
    for source in sources:
        args += source
    if start is not None:
        args.append(start)
    if counts is not None:
        args.append(counts.reshape(-1, lines, LANES))
    if after is not None:
        args.append(after)
    height = owned if counts is None else owned + TAIL
    return pl.pallas_call(
        functools.partial(
            segment_body, owned=owned, sources=len(sources), started=start is not None,
            counted=counts is not None, turn=turn, chips=chips,
        ),
        in_specs=smem(2) + vmem(len(args) - 2), out_specs=vmem(1)[0],
        out_shape=jax.ShapeDtypeStruct((height, 2 * width), dtype),
        compiler_params=params(12),
        cost_estimate=cost(4 * len(sources) * positions * owned * width),
    )(*args)


def home_body(spot_ref, ck_hbm, cv_hbm, *refs, owned, **sizes):
    sources = refs[:7]
    out_ref, ck, cv, sems = refs[7:]
    rows = pl.ds(pl.multiple_of(spot_ref[0] * owned, owned), owned)
    copies = [
        pltpu.make_async_copy(src.at[rows, :], dst, sems.at[i])
        for i, (src, dst) in enumerate(((ck_hbm, ck), (cv_hbm, cv)))
    ]
    for copy in copies:
        copy.start()
    segment_body(
        spot_ref, None, *sources, out_ref, owned=owned, sources=2, started=False, counted=True, **sizes
    )
    for copy in copies:
        copy.wait()


def home_sums(spot, chips, mine, other, counts, cent_k, cent_v, owned):
    positions, width = mine[0].shape
    f32 = jnp.float32
    lines = owned // LANES
    return pl.pallas_call(
        functools.partial(home_body, owned=owned, turn=0, chips=chips),
        in_specs=smem(1) + hbm(2) + vmem(7), out_specs=vmem(3),
        out_shape=[
            jax.ShapeDtypeStruct((owned + TAIL, 2 * width), f32),
            jax.ShapeDtypeStruct((owned, width), f32),
            jax.ShapeDtypeStruct((owned, width), f32),
        ],
        scratch_shapes=[pltpu.SemaphoreType.DMA((2,))],
        compiler_params=params(12), cost_estimate=cost(8 * positions * owned * width),
        name="home_sums",
    )(spot[0], cent_k, cent_v, *mine, *other, counts.reshape(-1, lines, LANES))


def dense_body(
    spot_ref, head_ref, *refs, scale, steps, span, block_len, heads
):
    asked = refs[:heads]
    (kc, vc, blocks, ks, vs, ids, sel_ref,
    peak_ref, whole_ref, acc_ref, q_ref, own_ref, query, held, best, sums, cache_bias, cache_hit, near_bias, light,
    kept_k, kept_v, list_v, list_s, sem) = refs[heads:]
    rows = q_ref.shape[0] // steps
    piece = rows // heads
    for d, ref in enumerate(asked):
        part = ref[...].astype(jnp.float32)
        source = lax.rem(head_ref[0] + heads - d, heads)
        for s in range(steps):
            at = pl.ds(pl.multiple_of(s * rows + source * piece, piece), piece)
            q_ref[at, :] = part[s * piece : (s + 1) * piece]
    query[...] = q_ref[...].astype(query.dtype)
    chosen = sel_ref.shape[1]
    eye = lax.broadcasted_iota(jnp.int32, (chosen, chosen), 0) == lax.broadcasted_iota(
        jnp.int32, (chosen, chosen), 1
    )
    wanted = jnp.concatenate(
        [
            jnp.broadcast_to(
                jnp.sum(
                    jnp.where(eye, sel_ref[s : s + 1, :].astype(jnp.float32), 0.0),
                    axis=1, keepdims=True,
                ),
                (chosen, LANES),
            )
            for s in range(steps)
        ],
        axis=0,
    )
    wanted = wanted.astype(jnp.int32).astype(jnp.int16)
    tell = jnp.where(
        lax.broadcasted_iota(jnp.int32, (8, steps * chosen), 0)
        == lax.broadcasted_iota(jnp.int32, (8, steps * chosen), 1) // chosen,
        1.0, 0.0,
    ).astype(jnp.bfloat16)

    def missing(names):
        names = names.astype(jnp.int16)
        same = jnp.concatenate(
            [
                jnp.where(
                    wanted == names[:, i : i + LANES], jnp.bfloat16(1), jnp.bfloat16(0)
                )
                for i in range(0, names.shape[1], LANES)
            ],
            axis=1,
        )
        found = jnp.dot(tell, same, preferred_element_type=jnp.float32)
        return jnp.where(found[:steps] > 0.5, 0.0, 1.0)

    owned = own_ref.shape[1]
    mine = spot_ref[0] * owned + lax.broadcasted_iota(jnp.int32, (1, owned), 1)
    own_ref[...] = (1.0 - missing(mine)) * NEG
    found = 1.0 - missing(blocks[...])
    count = found.shape[1]
    live = jnp.max(found, axis=0, keepdims=True)
    down = lax.broadcasted_iota(jnp.int32, (count, count), 0)
    along = lax.broadcasted_iota(jnp.int32, (count, count), 1)
    one, none = jnp.bfloat16(1), jnp.bfloat16(0)
    ahead = jnp.dot(
        jnp.broadcast_to(live, (8, count)).astype(jnp.bfloat16),
        jnp.where((down < along).astype(jnp.int16) > 0, one, none),
        preferred_element_type=jnp.float32,
    )[:1]
    place = jnp.where(live > 0.5, ahead, -1.0).astype(jnp.int32)
    chart = jnp.where((place == down).astype(jnp.int16) > 0, one, none)
    names = lax.broadcasted_iota(jnp.int32, (1, count), 1)
    table = jnp.concatenate(
        [(names // 64).astype(jnp.float32), (names % 64).astype(jnp.float32), found]
        + [jnp.zeros((6 - steps, count), jnp.float32)],
        axis=0,
    )
    packed = lax.dot_general(
        table.astype(jnp.bfloat16), chart, (((1,), (1,)), ((), ())),
        preferred_element_type=jnp.float32,
    )
    cache_hit[...] = packed[2 : 2 + steps]
    total = jnp.broadcast_to(jnp.sum(live, axis=1, keepdims=True), (1, count))
    list_v[...] = jnp.concatenate([64.0 * packed[:1] + packed[1:2], total], axis=0).astype(jnp.int32)
    listing = pltpu.make_async_copy(list_v, list_s, sem)
    listing.start()
    for at in range(0, ids.shape[1], 1024):
        near_bias[:, at : at + 1024] = missing(ids[:, at : at + 1024]) * NEG

    per = span // block_len
    widen = jnp.where(
        lax.broadcasted_iota(jnp.int32, (per, span), 0)
        == lax.broadcasted_iota(jnp.int32, (per, span), 1) // block_len,
        1.0, 0.0,
    ).astype(jnp.bfloat16)
    best[...] = jnp.full_like(best, NEG)
    sums[...] = jnp.zeros_like(sums)
    acc_ref[...] = jnp.zeros_like(acc_ref)

    def score(keys, at, shift, base):
        size = at.size
        found = lax.dot_general(
            query[...], keys[at, :], (((1,), (1,)), ((), ())), preferred_element_type=jnp.float32
        )
        found = found * scale
        found = jnp.concatenate(
            [found[s * rows : (s + 1) * rows] + shift[s : s + 1] for s in range(steps)], axis=0
        )
        held[:, pl.ds(pl.multiple_of(base + at.start, size), size)] = found
        top = best[...]
        for i in range(size // LANES):
            top = jnp.maximum(top, found[:, i * LANES : (i + 1) * LANES])
        best[...] = top

    def window(turn, span=span):
        return pl.ds(pl.multiple_of(turn * span, span), span)

    def score_near(turn, carry):
        score(ks, window(turn), near_bias[:, window(turn)], 0)
        return carry

    near = ks.shape[0]
    lax.fori_loop(0, near // span, score_near, 0)
    listing.wait()
    lively = list_s[1, 0]
    part = min(512, span)
    turns = (lively * block_len + part - 1) // part

    @pl.when(turns > 0)
    def _():
        last = window(turns - 1, part)
        kept_k[last, :] = jnp.zeros((part, kept_k.shape[1]), kept_k.dtype)
        kept_v[last, :] = jnp.zeros((part, kept_v.shape[1]), kept_v.dtype)

    def keep(n, carry):
        source = window(list_s[0, n], block_len)
        target = window(n, block_len)
        kept_k[target, :] = kc[source, :]
        kept_v[target, :] = vc[source, :]
        return carry

    lax.fori_loop(0, lively, keep, 0)

    def shift_cache(turn, carry):
        hit = cache_hit[:, pl.ds(pl.multiple_of(turn * per, per), per)].astype(jnp.bfloat16)
        cache_bias[:, window(turn)] = (
            1.0 - jnp.dot(hit, widen, preferred_element_type=jnp.float32)
        ) * NEG
        return carry

    lax.fori_loop(0, (lively + per - 1) // per, shift_cache, 0)

    def score_cache(turn, carry):
        at = window(turn, part)
        score(kept_k, at, cache_bias[:, at], near)
        return carry

    lax.fori_loop(0, turns, score_cache, 0)
    peak = jnp.max(best[...], axis=1, keepdims=True)
    peak_ref[...] = peak
    best[...] = jnp.broadcast_to(peak, best.shape)

    def weigh(values, at, base):
        tall, size = 64, at.size
        for r in range(0, best.shape[0], tall):
            top = best[r : r + tall, :]
            total = sums[r : r + tall, :]
            for i in range(0, size, LANES):
                lanes = pl.ds(pl.multiple_of(base + at.start + i, LANES), LANES)
                piece = jnp.exp2(held[r : r + tall, lanes] - top)
                total = total + piece
                light[r : r + tall, i : i + LANES] = piece.astype(light.dtype)
            sums[r : r + tall, :] = total
        acc_ref[...] += jnp.dot(
            light[:, :size], values[at, :], preferred_element_type=jnp.float32
        )

    def weigh_near(turn, carry):
        weigh(vs, window(turn), 0)
        return carry

    def weigh_cache(turn, carry):
        weigh(kept_v, window(turn, part), near)
        return carry

    lax.fori_loop(0, near // span, weigh_near, 0)
    lax.fori_loop(0, turns, weigh_cache, 0)
    whole_ref[...] = jnp.sum(sums[...], axis=1, keepdims=True)


def dense_part(spot, asked, cache_k, cache_v, blocks, near_k, near_v, ids, chosen, owned):
    width = asked[0].shape[1]
    heads = len(asked)
    rows = heads * asked[0].shape[0]
    steps = chosen.shape[0]
    far, near = cache_k.shape[0], near_k.shape[0]
    f32 = jnp.float32
    square = jax.ShapeDtypeStruct((rows, width), f32)
    span = min(2048, far, near)
    column = jax.ShapeDtypeStruct((rows, 1), f32)
    tile = pltpu.VMEM((rows, LANES), f32)
    return pl.pallas_call(
        functools.partial(
            dense_body, scale=width ** (-0.5) * LOG2E, steps=steps, span=span,
            block_len=far // blocks.shape[1], heads=heads,
        ),
        in_specs=smem(2) + vmem(heads + 7), out_specs=vmem(5),
        out_shape=[column, column, square, square, jax.ShapeDtypeStruct((steps, owned), f32)],
        scratch_shapes=[
            pltpu.VMEM((rows, width), asked[0].dtype), pltpu.VMEM((rows, far + near), f32), tile, tile,
            pltpu.VMEM((steps, far), f32), pltpu.VMEM((steps, blocks.shape[1]), f32),
            pltpu.VMEM((steps, near), f32), pltpu.VMEM((rows, span), jnp.bfloat16),
            pltpu.VMEM((far, width), cache_k.dtype), pltpu.VMEM((far, width), cache_v.dtype),
            pltpu.VMEM((2, blocks.shape[1]), jnp.int32), pltpu.SMEM((2, blocks.shape[1]), jnp.int32),
            pltpu.SemaphoreType.DMA(()),
        ],
        compiler_params=params(24),
        cost_estimate=cost(4 * rows * (far + near) * width),
        name="dense_part",
    )(*spot, *asked, cache_k, cache_v, blocks, near_k, near_v, ids, chosen)


def pieces_of(value, count):
    out = []
    for _ in range(count):
        piece = value.astype(jnp.bfloat16)
        out.append(piece)
        value = value - piece.astype(jnp.float32)
    return out


def finish_body(
    spot_ref, own_ref, *refs, owned, lines, steps, groups, scale, parcels
):
    came = refs[:parcels]
    (ck, cv, cc, bias_ref, q_ref, peak_ref, whole_ref, acc_ref,
     nk_ref, nv_ref, nc_ref, out_ref, res_ref, held) = refs[parcels:]
    width = ck.shape[1]
    sums = own_ref[:owned, :]
    tail = own_ref[owned:, :]
    for ref in came:
        sums = sums + ref[:owned, :].astype(jnp.float32)
        tail = tail + ref[owned:, :].astype(jnp.float32)
    pairs = 256.0 * tail[:, :LANES] + tail[:, LANES:]
    added = pairs[:lines]
    old_row = cc[:, pl.ds(pl.multiple_of(spot_ref[0] * owned, owned), owned)]
    total_row = old_row + jnp.concatenate([added[i : i + 1] for i in range(lines)], axis=1)
    nc_ref[...] = total_row
    eye = lax.broadcasted_iota(jnp.int32, (LANES, LANES), 0) == lax.broadcasted_iota(
        jnp.int32, (LANES, LANES), 1
    )

    def stand(row):
        return jnp.sum(jnp.where(eye, row, 0.0), axis=1, keepdims=True)

    def column(row):
        return jnp.concatenate(
            [stand(row[:, i : i + LANES]) for i in range(0, owned, LANES)], axis=0
        )

    old_col, new_col = column(old_row), column(total_row)
    new_k = (old_col * ck[...] + sums[:, :width]) / new_col
    new_v = (old_col * cv[...] + sums[:, width:]) / new_col
    nk_ref[...] = new_k
    nv_ref[...] = new_v
    log_row = jnp.log(total_row) * LOG2E
    query = q_ref[...].astype(jnp.bfloat16)
    scores = sum(
        lax.dot_general(
            query, piece, (((1,), (1,)), ((), ())), preferred_element_type=jnp.float32
        )
        for piece in reversed(pieces_of(new_k, 3))
    )
    scores = scores * scale + log_row
    rows_all = scores.shape[0]
    rows = rows_all // steps
    shift = bias_ref[...]
    scores = jnp.concatenate(
        [scores[s * rows : (s + 1) * rows] + shift[s : s + 1] for s in range(steps)], axis=0
    )
    before = peak_ref[...]
    peak = jnp.maximum(before, jnp.max(scores, axis=1, keepdims=True))
    weights = jnp.exp2(scores - peak)
    fade = jnp.exp2(before - peak)
    whole = whole_ref[...] * fade + jnp.sum(weights, axis=1, keepdims=True)
    (w_high, w_low), (v_high, v_low) = pieces_of(weights, 2), pieces_of(new_v, 2)
    acc = acc_ref[...] * fade
    for left, right in ((w_low, v_high), (w_high, v_low), (w_high, v_high)):
        acc = acc + jnp.dot(left, right, preferred_element_type=jnp.float32)
    res_ref[...] = acc / whole
    level = peak + jnp.log(whole) * LOG2E
    marks = [
        jnp.sum(jnp.where(eye, level[i * LANES : (i + 1) * LANES], 0.0), axis=0, keepdims=True)
        for i in range(rows_all // LANES)
    ]
    marks = [piece.astype(jnp.float32) for mark in marks for piece in pieces_of(mark, 3)]
    marks = jnp.concatenate(marks + [jnp.zeros((TAIL - len(marks), LANES), jnp.float32)], axis=0)
    share = rows // groups
    for g in range(groups):
        for s in range(steps):
            held[g, s * share : (s + 1) * share, :] = res_ref[
                s * rows + g * share : s * rows + (g + 1) * share, :
            ]
        held[g, steps * share :, :] = marks
    out_ref[...] = held[...].astype(out_ref.dtype)


def finish(spot, own, came, cent_k, cent_v, counts, bias, query, dense, groups, owned):
    width = cent_k.shape[1]
    rows = query.shape[0]
    steps = bias.shape[0]
    lines = owned // LANES
    height = steps * (rows // steps // groups) + TAIL
    f32 = jnp.float32
    args = [spot[0], own, *came, cent_k, cent_v, counts, bias, query, *dense]
    return pl.pallas_call(
        functools.partial(
            finish_body, owned=owned, lines=lines, steps=steps, groups=groups,
            scale=width ** (-0.5) * LOG2E, parcels=len(came),
        ),
        in_specs=smem(1) + vmem(len(args) - 1), out_specs=vmem(4),
        scratch_shapes=[
            pltpu.VMEM((rows, width), f32), pltpu.VMEM((groups, height, LANES), f32),
        ],
        out_shape=[
            jax.ShapeDtypeStruct((owned, width), f32),
            jax.ShapeDtypeStruct((owned, width), f32),
            jax.ShapeDtypeStruct((1, owned), f32),
            jax.ShapeDtypeStruct((groups, height, LANES), jnp.bfloat16),
        ],
        compiler_params=params(16), cost_estimate=cost(4e9),
        name="finish",
    )(*args)


def blend_body(spot_ref, in_ref, out_ref, *, steps, share, groups, rows):
    count = steps * share
    tiles = steps * rows // LANES
    spot = lax.broadcasted_iota(jnp.int32, (count, LANES), 0)
    lane = lax.broadcasted_iota(jnp.int32, (count, LANES), 1)
    wanted = (spot // share) * rows + spot_ref[0] * share + spot % share
    picks = [wanted == lane + i * LANES for i in range(tiles)]
    levels = []
    for g in range(groups):
        level = jnp.zeros((count, LANES), jnp.float32)
        marks = in_ref[g, count:, :].astype(jnp.float32)
        for i in range(tiles):
            mark = marks[3 * i : 3 * i + 1] + marks[3 * i + 1 : 3 * i + 2] + marks[3 * i + 2 : 3 * i + 3]
            level = level + jnp.where(picks[i], mark, 0.0)
        levels.append(jnp.sum(level, axis=1, keepdims=True))
    top = functools.reduce(jnp.maximum, levels)
    parts = [jnp.exp2(level - top) for level in levels]
    whole = functools.reduce(jnp.add, parts)
    acc = sum(part * in_ref[g, :count, :].astype(jnp.float32) for g, part in enumerate(parts))
    out_ref[...] = (acc / whole).astype(out_ref.dtype)


def blend(spot, packets, steps, share, groups, rows):
    return pl.pallas_call(
        functools.partial(blend_body, steps=steps, share=share, groups=groups, rows=rows),
        in_specs=smem(1) + vmem(1), out_specs=vmem(1)[0],
        out_shape=jax.ShapeDtypeStruct((steps * share, LANES), jnp.bfloat16),
        compiler_params=params(8),
        name="blend",
    )(spot[0], packets)


def spread(pairs):
    return [(2 * a + core, 2 * b + core) for a, b in pairs for core in (0, 1)]


def shards(
    stretch_keys, stretch_values, stretch_assign, centroid_keys, centroid_values, cluster_counts,
    cache_keys, cache_values, block_cluster, selected, queries,
):
    clusters, width = centroid_keys.shape[1:]
    groups = lax.axis_size("ctx")
    owned = clusters // groups
    chips = groups // 2
    swap = [(i, i ^ 1) for i in range(groups)]
    spot = tuple(lax.axis_index(name).astype(jnp.int32).reshape(1) for name in ("ctx", "head"))

    mine = (stretch_keys[0], stretch_values[0], stretch_assign)
    other_ids = lax.ppermute(mine[2], "ctx", swap)
    other = tuple(lax.ppermute(a, "ctx", swap) for a in mine[:2]) + (other_ids,)
    lead = chips - 1
    counts = chip_counts(mine[2], other[2], clusters)
    slot_a = segment_sums(spot, lead, chips, (mine,), None, None, owned, jnp.float32, after=counts)
    slot_a = segment_sums(spot, lead, chips, (other,), slot_a, counts, owned, jnp.bfloat16)

    def sums_for(turn):
        return segment_sums(spot, turn, chips, (mine, other), None, counts, owned, jnp.bfloat16)

    def move(a, pairs):
        return lax.ppermute(a, "ctx", spread(pairs))

    came = []
    for turn in range(lead, 0, -1):
        slot = slot_a if turn == lead else sums_for(turn)
        came.append(move(slot, [(i, target_of(i, turn, chips)) for i in range(chips)]))
    own, own_k, own_v = home_sums(
        spot, chips, mine, other, counts, centroid_keys[0], centroid_values[0], owned
    )
    heads = lax.axis_size("head")
    asked = list(by_head(spot, queries))
    for d in range(1, heads):
        asked[d] = lax.ppermute(asked[d], "head", [(i, (i + d) % heads) for i in range(heads)])
    steps = queries.shape[0]
    query_rows = heads * queries.shape[1]
    *dense, query, own_bias = dense_part(
        spot, asked, cache_keys[0], cache_values[0],
        block_cluster, *mine, selected[:, 0], owned,
    )
    new_keys, new_values, new_counts, packets = finish(
        spot, own, came, own_k, own_v, cluster_counts,
        own_bias, query, dense, groups, owned,
    )
    packets = lax.all_to_all(packets, "ctx", split_axis=0, concat_axis=0, tiled=True)
    share = query_rows // groups
    result = blend(spot, packets, steps, share, groups, query_rows)
    return (
        new_keys[None],
        new_values[None],
        new_counts,
        result.reshape(steps, 1, share, width),
    )


def solution(mesh):
    in_specs = (
        P("head", "ctx", None),
        P("head", "ctx", None),
        P("head", "ctx"),
        P("head", None, None),
        P("head", None, None),
        P("head", None),
        P("head", "ctx", None),
        P("head", "ctx", None),
        P("head", "ctx"),
        P(None, "head", None),
        P(None, "head", None, None),
    )
    out_specs = (
        P("head", "ctx", None),
        P("head", "ctx", None),
        P("head", "ctx"),
        P(None, "head", "ctx", None),
    )
    return jax.shard_map(shards, mesh=mesh, in_specs=in_specs, out_specs=out_specs, check_vma=False)
```
